32 devices in a mesh: dp: 16 (over z, x, core), tensor: 2 (over y).
Axes of the slice: x: 2, y: 2, z: 4, core: 2. Of those that a mesh axis runs over, the one named last changes fastest.
Arguments:
- inputs: bfloat16 [4096, 1792], P(('dp', 'tensor')), may hold values from -6 to 6
- cotangent: bfloat16 [4096, 1792], P(('dp', 'tensor')), may hold values from -6 to 6
- segments: int32 [16, 256], P('dp'), may hold values from 0 to 2, never falling along the last dimension, each value on 1 to 128 neighbouring positions
- slot_conv: int32 [294], replicated, may hold values from 0 to 367, as said below
- slot_mix: int32 [420], replicated, may hold values from 0 to 527, as said below
- slot_mlp: int32 [798], replicated, may hold values from 0 to 1007, as said below
- state_conv: float32 [3, 368, 32768], P(None, 'dp', 'tensor')
- state_mix: float32 [3, 528, 32768], P(None, 'dp', 'tensor'), as said below
- state_mlp: float32 [3, 1008, 32768], P(None, 'dp', 'tensor')
- small_state: float32 [3, 6, 1792], replicated, as said below
Outputs:
- result: bfloat16 [4096, 1792], P(('dp', 'tensor'))
- grad_input: float32 [4096, 1792], P(('dp', 'tensor'))
- new_conv: float32 [3, 368, 32768], P(None, 'dp', 'tensor')
- new_mix: float32 [3, 528, 32768], P(None, 'dp', 'tensor')
- new_mlp: float32 [3, 1008, 32768], P(None, 'dp', 'tensor')
- new_small: float32 [2, 6, 1792], replicated
- small_update: float32 [6, 1792], replicated
The draws below stay inside these ranges and needn't reach their ends.
Inputs may be any that keep to these rules, and one draw needn't show every extreme that they name: `slot_conv`: distinct slot numbers; the owner of a unit is the dp index slot // 23, so that every owner holds at most 23 units and one owner holds exactly 23. The first and the last slot are always used. `slot_mix`: distinct slot numbers; the owner of a unit is slot // 33, at most 33 units an owner, one owner holding exactly 33. The first and the last slot are always used. `slot_mlp`: distinct slot numbers; the owner of a unit is slot // 63, at most 63 units an owner, one owner holding exactly 63. The first and the last slot are always used. `state_mix`: the second moments (index 2) are positive. `small_state`: the second moments (index 2) are positive.
All inputs are finite; a program needn't handle non-finite values.
Results may differ from the reference program's by a relative error of at most 0.025.
Values may be sent and summed in bfloat16 or wider, within the bound.
A program may use at most 384 MiB of HBM per device.

```python
import math
import jax
import jax.numpy as jnp
import numpy as np
from jax import lax

D = 1792
HEADS = 16
FEAT = 16
FF = 4864
WINDOW = 64
TAPS = 3
STEP = 5
UNIT = 16384
SEQ = 256
HEAD = 112
TOKENS = 4096
UC = 294
UM = 420
UF = 798
CAPC = 23
CAPM = 33
CAPF = 63
N_DP = 16
N_TENSOR = 2


def pick_slots(key, units, capacity):
    slot_total = N_DP * capacity
    owner_full = jax.random.randint(jax.random.fold_in(key, 1), (), 0, N_DP)
    priority = jax.random.permutation(jax.random.fold_in(key, 2), slot_total).astype(jnp.int32)
    slot_ids = jnp.arange(slot_total, dtype=jnp.int32)
    owner_ids = slot_ids // capacity
    forced = (owner_ids == owner_full) | (slot_ids == 0) | (slot_ids == slot_total - 1)
    ranking = priority + slot_total * forced.astype(jnp.int32)
    _, chosen = lax.top_k(ranking, units)
    shuffle = jax.random.permutation(jax.random.fold_in(key, 3), units)
    return chosen[shuffle].astype(jnp.int32)


def draw_slot_conv(key, part):
    return pick_slots(jax.random.fold_in(key, 11), UC, CAPC)


def draw_slot_mix(key, part):
    return pick_slots(jax.random.fold_in(key, 12), UM, CAPM)


def draw_slot_mlp(key, part):
    return pick_slots(jax.random.fold_in(key, 13), UF, CAPF)


def state_block(key, row_total, row_scale, grad_scale):
    sub_keys = jax.random.split(key, 3)
    width_all = N_TENSOR * UNIT
    base_draw = jax.random.normal(sub_keys[0], (row_total, width_all), jnp.float32)
    master = base_draw * row_scale[:, None]
    moment_one = jax.random.normal(sub_keys[1], (row_total, width_all), jnp.float32) * (0.11 * grad_scale)
    moment_two = jax.random.uniform(sub_keys[2], (row_total, width_all), jnp.float32, 0.3, 3.0) * (0.053 * grad_scale * grad_scale)
    return jnp.stack([master, moment_one, moment_two])


def draw_state_conv(key, part):
    row_total = N_DP * CAPC
    grad_scale = 3.0 * 0.125 * math.sqrt(TOKENS) / N_DP
    return state_block(jax.random.fold_in(key, 21), row_total, jnp.full((row_total,), 8.0 * D ** (-0.5), jnp.float32), grad_scale)


def draw_state_mix(key, part):
    row_total = N_DP * CAPM
    slots = pick_slots(jax.random.fold_in(key, 12), UM, CAPM)
    outward = D * (D // N_TENSOR) // UNIT
    row_scale = jnp.full((row_total,), 4.0 * D ** (-0.5), jnp.float32).at[slots[UM - outward:]].set(16.0 * D ** (-0.5))
    grad_scale = 1.1 * 0.25 * math.sqrt(TOKENS) / N_DP
    return state_block(jax.random.fold_in(key, 22), row_total, row_scale, grad_scale)


def draw_state_mlp(key, part):
    row_total = N_DP * CAPF
    grad_scale = 0.42 * 0.5 * math.sqrt(TOKENS) / N_DP
    return state_block(jax.random.fold_in(key, 23), row_total, jnp.full((row_total,), 2.0 * D ** (-0.5), jnp.float32), grad_scale)


def draw_small_state(key, part):
    sub_keys = jax.random.split(jax.random.fold_in(key, 31), 3)
    rows_all = 3 + TAPS
    noise = jax.random.normal(sub_keys[0], (rows_all, D), jnp.float32)
    row_ids = jnp.arange(rows_all)[:, None]
    params = 8.0 * (jnp.where(row_ids < 3, 1.0 + 0.1 * noise, 0.5 * noise) + (row_ids == 3).astype(jnp.float32))
    grad_scale = 2.5 * 0.125 * math.sqrt(TOKENS) / N_DP
    moment_one = jax.random.normal(sub_keys[1], (rows_all, D), jnp.float32) * (0.11 * grad_scale)
    moment_two = jax.random.uniform(sub_keys[2], (rows_all, D), jnp.float32, 0.3, 3.0) * (0.053 * grad_scale * grad_scale)
    return jnp.stack([params, moment_one, moment_two])


def steps_of(key, dims, cuts, smallest, high):
    level = 1.0
    for axis_at, blocks in cuts:
        heights = jax.random.uniform(jax.random.fold_in(jax.random.fold_in(key, 6), axis_at), (blocks,), jnp.float32, smallest / len(cuts), high / len(cuts))
        level = level * jnp.repeat(jnp.exp(heights), dims[axis_at] // blocks).reshape((-1,) + (1,) * (len(dims) - 1 - axis_at))
    return level


def length_profile(count, total, bound, slope):
    loads = [(1 << 20) // math.isqrt(grade ** slope) + 1 for grade in range(2, count + 1)]
    spare, holding = total - bound - (count - 1), [1] * (count - 1)
    while spare > 0:
        free = [i for i in range(count - 1) if holding[i] < bound]
        pool, remaining = sum([loads[i] for i in free]), spare
        for i in free:
            addition = min(bound - holding[i], max(1, remaining * loads[i] // pool), spare)
            holding[i] = holding[i] + addition
            spare = spare - addition
    return np.array([bound] + holding)


def uneven_parts(rng, number_of, total, bound, slope):
    if number_of == 2:
        one = jax.random.randint(rng, (), max(1, total - bound), min(bound, total - 1) + 1)
        return jnp.stack([one, total - one])
    tallies = jnp.asarray(length_profile(number_of, total, bound, slope), jnp.int32)
    twos = (number_of - 1) // 2
    donor, receiver = tallies[1:1 + 2 * twos:2], tallies[2:2 + 2 * twos:2]
    slack = jnp.minimum(donor - 1, bound - receiver)
    passed = jax.random.randint(jax.random.fold_in(rng, 1), (twos,), 0, 1 << 20) % (slack + 1)
    tallies = tallies.at[1:1 + 2 * twos:2].set(donor - passed).at[2:2 + 2 * twos:2].set(receiver + passed)
    return tallies[jax.random.permutation(jax.random.fold_in(rng, 2), number_of)]


def gaussian(own_key, dims, width, limit, shards=(), held_as=jnp.bfloat16):
    level = steps_of(own_key, dims, shards, -0.22, 0.18) if shards else 1.0
    entries = jax.random.normal(own_key, dims, jnp.float32) * width * level
    return jnp.minimum(jnp.maximum(entries, -limit), limit).astype(held_as)


def setup_inputs(seed: int = 0) -> dict:
    key_of = jax.random.split(jax.random.key(seed), 11)
    inputs = gaussian(key_of[0], (TOKENS, D), 1.0, 6.0, ((0, 32),))
    cotangent = gaussian(key_of[1], (TOKENS, D), 1.0, 6.0, ((0, 32),))
    segments = jax.vmap(lambda own: jnp.searchsorted(jnp.cumsum(uneven_parts(own, 3, SEQ, SEQ // 2, 0)), jnp.arange(SEQ), side="right"))(jax.random.split(key_of[2], N_DP)).reshape((N_DP, SEQ)).astype(jnp.int32)
    slot_conv = draw_slot_conv(jax.random.fold_in(key_of[10], 71), 0)
    slot_mix = draw_slot_mix(jax.random.fold_in(key_of[10], 71), 0)
    slot_mlp = draw_slot_mlp(jax.random.fold_in(key_of[10], 71), 0)
    state_conv = draw_state_conv(jax.random.fold_in(key_of[10], 71), 0)
    state_mix = draw_state_mix(jax.random.fold_in(key_of[10], 71), 0)
    state_mlp = draw_state_mlp(jax.random.fold_in(key_of[10], 71), 0)
    small_state = draw_small_state(jax.random.fold_in(key_of[10], 71), 0)
    return {"inputs": inputs, "cotangent": cotangent, "segments": segments, "slot_conv": slot_conv, "slot_mix": slot_mix, "slot_mlp": slot_mlp, "state_conv": state_conv, "state_mix": state_mix, "state_mlp": state_mlp, "small_state": small_state}


PRECISE = lax.Precision.HIGHEST
NORM_EPS = 1e-05
BETA_ONE = 0.9
BETA_TWO = 0.95
ADAM_EPS = 1e-08
LEARN_RATE = 0.02
SMALL_RATE = 0.16
WEIGHT_DECAY = 0.1
NEG_FILL = -1e+30
GROUP_SCALES = (0.125, 0.25, 0.5)
SMALL_SCALE = 0.125

@jax.custom_vjp
def low(v):
    return lax.optimization_barrier(v.astype(jnp.bfloat16)).astype(jnp.float32)

@jax.custom_vjp
def low_back(v):
    return v

def low_keep(v):
    return (low(v), None)

def low_pass(kept, grad):
    return (grad,)

def back_keep(v):
    return (v, None)

def back_low(kept, grad):
    return (low(grad),)
low.defvjp(low_keep, low_pass)
low_back.defvjp(back_keep, back_low)

def mat_mul(left, right):
    return jnp.einsum('nsd,de->nse', left, right, precision=PRECISE)

def rms_norm(values, gain):
    return values * lax.rsqrt(lax.optimization_barrier(jnp.mean(values * values, axis=-1, keepdims=True)) + NORM_EPS) * gain

def shifted(values, steps):
    return jnp.pad(values, ((0, 0), (steps, 0), (0, 0)))[:, :values.shape[1]]

def attend(pieces):
    query_f, key_f, query_s, key_s, values_v, seg_ids = pieces
    length = seg_ids.shape[0]
    positions = jnp.arange(length)
    causal = (positions[:, None] >= positions[None, :]) & (seg_ids[:, None] == seg_ids[None, :])
    lin_mask = causal.astype(jnp.float32)
    inside = causal & (positions[:, None] - positions[None, :] < WINDOW)
    lin_score = low_back(jnp.einsum('shf,thf->hst', query_f, key_f, precision=PRECISE) / math.sqrt(FEAT))
    kernel = (1.0 + lin_score + 0.5 * lin_score * lin_score) * lin_mask
    lin_prob = low(kernel / lax.optimization_barrier(jnp.sum(kernel, axis=-1, keepdims=True)))
    win_score = low_back(jnp.einsum('shd,thd->hst', query_s, key_s, precision=PRECISE) / math.sqrt(HEAD))
    win_peak = lax.optimization_barrier(jnp.max(jnp.where(inside, win_score, NEG_FILL), axis=-1, keepdims=True))
    win_exp = jnp.exp(jnp.where(inside, win_score - win_peak, NEG_FILL))
    win_prob = low(win_exp / lax.optimization_barrier(jnp.sum(win_exp, axis=-1, keepdims=True)))
    return jnp.einsum('hst,thd->shd', lin_prob, values_v, precision=PRECISE) + jnp.einsum('hst,thd->shd', win_prob, values_v, precision=PRECISE)

def block_forward(matrices, params, x_values, seg_ids):
    conv_w, mix_w, mlp_w = matrices
    seq_count, length, _ = x_values.shape
    normed_one = low(rms_norm(x_values, params[0]))
    value_c = low_back(mat_mul(normed_one, conv_w[0]))
    gate_c = low_back(mat_mul(normed_one, conv_w[1]))
    mixed_c = params[3] * value_c
    for shift_by in range(1, TAPS):
        earlier = jnp.pad(seg_ids, ((0, 0), (shift_by, 0)), constant_values=-1)[:, :length]
        same_doc = (earlier == seg_ids).astype(jnp.float32)[..., None]
        mixed_c = mixed_c + params[3 + shift_by] * shifted(value_c, shift_by) * same_doc
    gated_conv = low_back(low(mixed_c * gate_c))
    hidden_one = x_values + low_back(mat_mul(gated_conv, conv_w[2]))
    normed_two = low(rms_norm(hidden_one, params[1]))
    query_f = low_back(low(mat_mul(normed_two, mix_w[0]))).reshape(seq_count, length, HEADS, FEAT)
    key_f = low_back(low(mat_mul(normed_two, mix_w[1]))).reshape(seq_count, length, HEADS, FEAT)
    query_s = low_back(low(mat_mul(normed_two, mix_w[2]))).reshape(seq_count, length, HEADS, HEAD)
    key_s = low_back(low(mat_mul(normed_two, mix_w[3]))).reshape(seq_count, length, HEADS, HEAD)
    values_v = low_back(low(mat_mul(normed_two, mix_w[4]))).reshape(seq_count, length, HEADS, HEAD)
    attended = lax.map(jax.checkpoint(attend), (query_f, key_f, query_s, key_s, values_v, seg_ids))
    mix_out = low_back(low(attended.reshape(seq_count, length, D)))
    hidden_two = hidden_one + low_back(mat_mul(mix_out, mix_w[5]))
    normed_three = low(rms_norm(hidden_two, params[2]))
    gate_proj = low_back(mat_mul(normed_three, mlp_w[0]))
    up_proj = low_back(mat_mul(normed_three, mlp_w[1]))
    activated = low(jax.nn.silu(gate_proj) * up_proj)
    return hidden_two + low_back(mat_mul(activated, mlp_w[2]))

def unpack(master_rows, slots, shapes, splits):
    halves = []
    for which_half in range(N_TENSOR):
        flat_rows = master_rows[slots, which_half * UNIT:(which_half + 1) * UNIT].reshape(-1)
        pieces = []
        offset = 0
        for dims_pair in shapes:
            elements = dims_pair[0] * dims_pair[1]
            pieces.append(flat_rows[offset:offset + elements].reshape(dims_pair))
            offset += elements
        halves.append(pieces)
    return [jnp.concatenate([halves[which_half][index_m] for which_half in range(N_TENSOR)], axis=splits[index_m]) for index_m in range(len(shapes))]

def pack_units(gradients, slots, splits, slot_rows):
    packed = jnp.zeros((slot_rows, N_TENSOR * UNIT), jnp.float32)
    for which_half in range(N_TENSOR):
        flat_rows = jnp.concatenate([jnp.split(gradient, N_TENSOR, axis=splits[index_m])[which_half].reshape(-1) for index_m, gradient in enumerate(gradients)])
        packed = packed.at[slots, which_half * UNIT:(which_half + 1) * UNIT].set(flat_rows.reshape(-1, UNIT))
    return packed

def adam_step(opt_state, gradient, rate):
    moment_one = BETA_ONE * opt_state[1] + (1.0 - BETA_ONE) * gradient
    moment_two = BETA_TWO * opt_state[2] + (1.0 - BETA_TWO) * gradient * gradient
    step_size = moment_one / (1.0 - BETA_ONE ** STEP) / (jnp.sqrt(moment_two / (1.0 - BETA_TWO ** STEP)) + ADAM_EPS)
    return jnp.stack([opt_state[0] - rate * (step_size + WEIGHT_DECAY * opt_state[0]), moment_one, moment_two])

def reference(inputs, cotangent, segments, slot_conv, slot_mix, slot_mlp, state_conv, state_mix, state_mlp, small_state):
    half_width = D // N_TENSOR
    feat_cols = HEADS * FEAT // N_TENSOR
    ff_half = FF // N_TENSOR
    buckets = ((state_conv, slot_conv, [(D, half_width), (D, half_width), (half_width, D)], [1, 1, 0]), (state_mix, slot_mix, [(D, feat_cols), (D, feat_cols), (D, half_width), (D, half_width), (D, half_width), (half_width, D)], [1, 1, 1, 1, 1, 0]), (state_mlp, slot_mlp, [(D, ff_half), (D, ff_half), (ff_half, D)], [1, 1, 0]))
    masters = [unpack(bucket[0][0], bucket[1], bucket[2], bucket[3]) for bucket in buckets]
    x_rows = inputs.astype(jnp.float32).reshape(N_DP, SEQ, D)

    def forward(matrices, params, x_values):
        scaled = [[low(matrix * scale) for matrix in group] for group, scale in zip(matrices, GROUP_SCALES)]
        return block_forward(scaled, params * SMALL_SCALE, x_values, segments)
    out_rows, pullback = jax.vjp(forward, masters, small_state[0], x_rows)
    grad_mats, grad_params, grad_x = pullback(cotangent.astype(jnp.float32).reshape(N_DP, SEQ, D))
    new_states = [adam_step(bucket[0], pack_units(grad_bucket, bucket[1], bucket[3], bucket[0].shape[1]) / N_DP, LEARN_RATE) for bucket, grad_bucket in zip(buckets, grad_mats)]
    small_new = adam_step(small_state, grad_params / N_DP, SMALL_RATE)
    return (out_rows.reshape(TOKENS, D).astype(jnp.bfloat16), grad_x.reshape(TOKENS, D), new_states[0], new_states[1], new_states[2], small_new[1:], small_new[0] - small_state[0])
```

```python
import math

import functools

import jax
import jax.numpy as jnp
from jax import lax
from jax.experimental import pallas as pl
from jax.experimental.pallas import tpu as pltpu
from jax.sharding import PartitionSpec as P

LANES = 128

D = 1792
HEADS = 16
FEAT = 16
FF = 4864
WINDOW = 64
TAPS = 3
STEP = 5
HEAD = 112


NORM_EPS = 1e-05
BETA_ONE = 0.9
BETA_TWO = 0.95
ADAM_EPS = 1e-08
LEARN_RATE = 0.02
SMALL_RATE = 0.16
WEIGHT_DECAY = 0.1
NEG_FILL = -1e30
CONV_SCALE = 0.125
MIX_SCALE = 0.25
MLP_SCALE = 0.5
SMALL_SCALE = 0.125


def norm_rows(values, gain):
    return values * lax.rsqrt(jnp.mean(values * values, axis=-1, keepdims=True) + NORM_EPS) * gain


def norm_back(values, gain, upstream):
    _, pullback = jax.vjp(norm_rows, values, gain)
    return pullback(upstream)


def product(left, right):
    return jnp.dot(left, right, preferred_element_type=jnp.float32)


def product_left(left, right):
    return lax.dot_general(
        left, right, (((0,), (0,)), ((), ())), preferred_element_type=jnp.float32
    )


def product_right(left, right):
    return lax.dot_general(
        left, right, (((1,), (1,)), ((), ())), preferred_element_type=jnp.float32
    )


def swap(values, axis, bit):
    size = lax.axis_size(axis)
    return lax.ppermute(values, axis, [(i, i ^ bit) for i in range(size)])


def gather_rows(piece_rows):
    other = swap(piece_rows, "tensor", 1)
    first = lax.axis_index("tensor") == 0
    return jnp.concatenate(
        [jnp.where(first, piece_rows, other), jnp.where(first, other, piece_rows)]
    )


def sum_rows(piece_rows):
    rows = piece_rows.shape[0] // 2
    at = lax.axis_index("tensor")
    halves = piece_rows.astype(jnp.bfloat16).reshape(2, rows, piece_rows.shape[1])
    other = swap(lax.dynamic_index_in_dim(halves, 1 - at, 0, False), "tensor", 1)
    mine = lax.dynamic_index_in_dim(halves, at, 0, False)
    return mine.astype(jnp.float32) + other.astype(jnp.float32)


def delayed(values, steps):
    return jnp.pad(values, ((steps, 0), (0, 0)))[: values.shape[0]]


def advanced(values, steps):
    return jnp.pad(values, ((0, steps), (0, 0)))[steps:]


def lay_body(first, nu, blocks, m, slots_ref, pooled_ref, out_ref, buf, stage, sem):
    step = pl.program_id(0)
    per_step = nu * blocks

    def fetch(at, half):
        for q in range(per_step):
            pltpu.make_async_copy(
                pooled_ref.at[slots_ref[first + at * per_step + q]], buf.at[half, q], sem.at[half]
            ).start()

    @pl.when(step == 0)
    def _():
        fetch(0, 0)

    @pl.when(step + 1 < pl.num_programs(0))
    def _():
        fetch(step + 1, (step + 1) % 2)

    half = step % 2
    pltpu.make_async_copy(pooled_ref.at[pl.ds(0, per_step)], buf.at[half], sem.at[half]).wait()
    depth = buf.shape[2]
    rows = nu * depth // m
    for block in range(blocks):
        if m == 1:
            for q in range(nu):
                at = (block * nu + q) * depth
                out_ref[at : at + depth, :] = buf[half, block * nu + q]
            continue
        for q in range(nu):
            stage[q * depth : (q + 1) * depth, :] = buf[half, block * nu + q].astype(jnp.float32)
        for c in range(m):
            out_ref[block * rows : (block + 1) * rows, c * LANES : (c + 1) * LANES] = stage[
                pl.ds(c, rows, stride=m), :
            ].astype(jnp.bfloat16)


def lay_out(pooled, slots, first, count, width, nu, blocks):
    depth = pooled.shape[1]
    m = width // LANES
    rows = nu * blocks * depth // m
    steps = count // (nu * blocks)
    assert steps * nu * blocks == count
    return pl.pallas_call(
        functools.partial(lay_body, first, nu, blocks, m),
        grid_spec=pltpu.PrefetchScalarGridSpec(
            num_scalar_prefetch=1,
            grid=(steps,),
            in_specs=[pl.BlockSpec(memory_space=pl.ANY)],
            out_specs=pl.BlockSpec((rows, width), lambda i, s: (i, 0)),
            scratch_shapes=[
                pltpu.VMEM((2, nu * blocks, depth, LANES), jnp.bfloat16),
                pltpu.VMEM((nu * depth, LANES), jnp.float32),
                pltpu.SemaphoreType.DMA((2,)),
            ],
        ),
        out_shape=jax.ShapeDtypeStruct((steps * rows, width), jnp.bfloat16),
        cost_estimate=pl.CostEstimate(
            flops=0, bytes_accessed=4 * count * depth * LANES, transcendentals=0
        ),
        name=f"lay_{width}_{count}",
    )(slots, pooled)


def grad_body(first, nu, m, has_old, slots_ref, u_ref, d_ref, *rest):
    out_ref, stage, buf, sem = rest[1:] if has_old else rest
    step = pl.program_id(0)
    half = step % 2
    depth = buf.shape[2]
    rows = u_ref.shape[1]

    def drain(which):
        pltpu.make_async_copy(out_ref.at[pl.ds(0, nu)], buf.at[which], sem.at[which]).wait()

    @pl.when(step >= 2)
    def _():
        drain(half)

    for c in range(0, m, 2):
        wide = min(2, m - c)
        piece = lax.dot_general(
            u_ref[...],
            d_ref[:, c * LANES : (c + wide) * LANES],
            (((0,), (0,)), ((), ())),
            preferred_element_type=jnp.float32,
        )
        for k in range(wide):
            part = piece[:, k * LANES : (k + 1) * LANES]
            if m == 1:
                stage[...] = part
            else:
                stage[pl.ds(c + k, rows, stride=m), :] = part
    for q in range(nu):
        buf[half, q] = stage[q * depth : (q + 1) * depth, :].astype(jnp.bfloat16)
    for q in range(nu):
        pltpu.make_async_copy(
            buf.at[half, q], out_ref.at[slots_ref[first + step * nu + q]], sem.at[half]
        ).start()

    @pl.when(step + 1 == pl.num_programs(0))
    def _():
        drain(half)

        @pl.when(step >= 1)
        def _():
            drain(1 - half)


def grad_units(old, slot_rows, slots, first, u, d, rows):
    tokens, height = u.shape
    width = d.shape[1]
    m = width // LANES
    depth = LANES
    nu = rows * m // depth
    steps = height // rows
    has_old = old is not None
    shape = jax.ShapeDtypeStruct((slot_rows, depth, LANES), jnp.bfloat16)
    specs = [
        pl.BlockSpec((tokens, rows), lambda i, s: (0, i)),
        pl.BlockSpec((tokens, width), lambda i, s: (0, 0)),
    ]
    operands = [slots, u, d]
    if has_old:
        specs.append(pl.BlockSpec(memory_space=pl.ANY))
        operands.append(old)
    return pl.pallas_call(
        functools.partial(grad_body, first, nu, m, has_old),
        grid_spec=pltpu.PrefetchScalarGridSpec(
            num_scalar_prefetch=1,
            grid=(steps,),
            in_specs=specs,
            out_specs=pl.BlockSpec(memory_space=pl.ANY),
            scratch_shapes=[
                pltpu.VMEM((nu * depth, LANES), jnp.float32),
                pltpu.VMEM((2, nu, depth, LANES), jnp.bfloat16),
                pltpu.SemaphoreType.DMA((2,)),
            ],
        ),
        out_shape=shape,
        input_output_aliases={3: 0} if has_old else {},
        cost_estimate=pl.CostEstimate(
            flops=2 * tokens * height * width,
            bytes_accessed=2 * height * width + 2 * tokens * (height + width),
            transcendentals=0,
        ),
        name=f"grad_{height}_{width}",
    )(*operands)


def bits_of(owners):
    return owners.bit_length() - 1


def chunks_of(total, most):
    number = -(-total // most)
    base, extra = divmod(total, number)
    out, at = [], 0
    for k in range(number):
        size = base + (1 if k < extra else 0)
        out.append((at, size))
        at += size
    return out


def slot_rows_of(slots, owners, cap, chunks):
    owner, at = slots // cap, slots % cap
    row = jnp.zeros_like(slots)
    for start, size in chunks:
        inside = (at >= start) & (at < start + size)
        here = start * owners + (owner % 2) * (owners // 2 * size) + (owner // 2) * size + at - start
        row = jnp.where(inside, here, row)
    return row


def scatter_sum(units, owners, cap, chunks):
    me = lax.axis_index("dp")
    tail = units.shape[1:]
    summed = []
    for number, (start, size) in enumerate(chunks):
        bits = list(range(bits_of(owners)))
        order = list(bits)
        if number == len(chunks) - 1 and len(order) > 2:
            order[1], order[2] = order[2], order[1]
        half = owners // 2 * size
        pair = units[start * owners : (start + size) * owners].reshape(2, half, *tail)
        left = bits[1:]
        mine = (me // 1) % 2
        send = lax.dynamic_index_in_dim(pair, 1 - mine, 0, False)
        kept = lax.dynamic_index_in_dim(pair, mine, 0, False).reshape(owners // 2, size, *tail)
        for step, b in enumerate(order):
            got = swap(send, "dp", 1 << b).reshape(kept.shape)
            if step + 1 == len(order):
                summed.append((kept.astype(jnp.float32) + got.astype(jnp.float32))[0])
                break
            now = (kept.astype(jnp.float32) + got.astype(jnp.float32)).astype(jnp.bfloat16)
            nxt = order[step + 1]
            low = left.index(nxt)
            split = now.reshape(-1, 2, 1 << low, size, *tail)
            mine = (me // (1 << nxt)) % 2
            send = lax.dynamic_index_in_dim(split, 1 - mine, 1, False)
            kept = lax.dynamic_index_in_dim(split, mine, 1, False)
            left.remove(nxt)
            kept = kept.reshape(1 << len(left), size, *tail)
            send = send.reshape(kept.shape)
    return jnp.concatenate(summed)


def total_of(values, owners):
    for b in range(bits_of(owners)):
        values = values + swap(values, "dp", 1 << b)
    return values + swap(values, "tensor", 1)


def adam_values(master, one, two, gradient, rate):
    moment_one = BETA_ONE * one + (1.0 - BETA_ONE) * gradient
    moment_two = BETA_TWO * two + (1.0 - BETA_TWO) * gradient * gradient
    step_size = (
        moment_one
        / (1.0 - BETA_ONE**STEP)
        / (jnp.sqrt(moment_two / (1.0 - BETA_TWO**STEP)) + ADAM_EPS)
    )
    return master - rate * (step_size + WEIGHT_DECAY * master), moment_one, moment_two


def adam_step(opt_state, gradient, rate):
    return jnp.stack(adam_values(opt_state[0], opt_state[1], opt_state[2], gradient, rate))


def adam_body(state_ref, gradient_ref, out_ref):
    new = adam_values(state_ref[0], state_ref[1], state_ref[2], gradient_ref[...], LEARN_RATE)
    for k in range(3):
        out_ref[k] = new[k]


def adam_units(state, summed, slots, scale):
    cap, unit_width = state.shape[1:]
    mine = lax.axis_index("dp") * cap + jnp.arange(cap, dtype=jnp.int32)
    used = jnp.any(mine[:, None] == slots[None, :], axis=1)
    gradient = jnp.where(used[:, None, None], summed * scale, 0.0).reshape(cap, unit_width)
    block = 2048
    return pl.pallas_call(
        adam_body,
        grid=(unit_width // block,),
        in_specs=[
            pl.BlockSpec((3, cap, block), lambda i: (0, 0, i)),
            pl.BlockSpec((cap, block), lambda i: (0, i)),
        ],
        out_specs=pl.BlockSpec((3, cap, block), lambda i: (0, 0, i)),
        out_shape=jax.ShapeDtypeStruct(state.shape, jnp.float32),
        name=f"adam_{cap}",
    )(state, gradient)


def gather_units(state, scale):
    cap, unit_width = state.shape[1:]
    own = (state[0] * scale).reshape(cap, unit_width // LANES, LANES).astype(jnp.bfloat16)
    return lax.all_gather(own, "dp", axis=0, tiled=True)


def attend(query_f, key_f, query_s, key_s, lin_mask, win_mask):
    lin_score = jnp.einsum(
        "shf,thf->hst", query_f, key_f, preferred_element_type=jnp.float32
    ) / math.sqrt(FEAT)
    kernel = (1.0 + lin_score + 0.5 * lin_score * lin_score) * lin_mask
    lin_denom = jnp.sum(kernel, axis=-1, keepdims=True)
    lin_prob = kernel / lin_denom
    win_score = jnp.einsum(
        "shd,thd->hst", query_s, key_s, preferred_element_type=jnp.float32
    ) / math.sqrt(HEAD)
    inside = win_mask > 0
    win_peak = jnp.max(jnp.where(inside, win_score, NEG_FILL), axis=-1, keepdims=True)
    win_exp = jnp.exp(jnp.where(inside, win_score - win_peak, NEG_FILL))
    win_prob = win_exp / jnp.sum(win_exp, axis=-1, keepdims=True)
    return (lin_score, lin_denom, lin_prob, win_prob)


def per_device(
    inputs,
    cotangent,
    segments,
    slot_conv,
    slot_mix,
    slot_mlp,
    state_conv,
    state_mix,
    state_mlp,
    small_state,
):
    tensor_size = lax.axis_size("tensor")
    owners = lax.axis_size("dp")
    half_width = D // tensor_size
    local_heads = HEADS // tensor_size
    feat_cols = local_heads * FEAT
    ff_half = FF // tensor_size
    unit_width = state_conv.shape[2]
    cap_conv = state_conv.shape[1]
    cap_mix = state_mix.shape[1]
    cap_mlp = state_mlp.shape[1]
    pooled = (
        gather_units(state_conv, CONV_SCALE),
        gather_units(state_mix, MIX_SCALE),
        gather_units(state_mlp, MLP_SCALE),
    )
    per = D * LANES // unit_width
    narrow, middle = per * feat_cols // LANES, per * half_width // LANES
    wide = per * ff_half // LANES
    conv_pair = lay_out(pooled[0], slot_conv, 0, 2 * middle, half_width, 7, 2)
    conv_w = [
        conv_pair[:D],
        conv_pair[D:],
        lay_out(pooled[0], slot_conv, 2 * middle, middle, D, 7, 2),
    ]
    feat_pair = lay_out(pooled[1], slot_mix, 0, 2 * narrow, feat_cols, 7, 1)
    mix_trio = lay_out(pooled[1], slot_mix, 2 * narrow, 3 * middle, half_width, 7, 2)
    mix_w = [
        feat_pair[:D],
        feat_pair[D:],
        mix_trio[:D],
        mix_trio[D : 2 * D],
        mix_trio[2 * D :],
        lay_out(pooled[1], slot_mix, 2 * narrow + 3 * middle, middle, D, 7, 2),
    ]
    mlp_pair = lay_out(pooled[2], slot_mlp, 0, 2 * wide, ff_half, 19, 1)
    mlp_w = [
        mlp_pair[:D],
        mlp_pair[D:],
        lay_out(pooled[2], slot_mlp, 2 * wide, wide, D, 7, 2),
    ]
    chunks_mlp = chunks_of(cap_mlp, 16)
    chunks_mix = chunks_of(cap_mix, 11)
    chunks_conv = chunks_of(cap_conv, 8)
    rows_mlp = slot_rows_of(slot_mlp, owners, cap_mlp, chunks_mlp)
    rows_mix = slot_rows_of(slot_mix, owners, cap_mix, chunks_mix)
    rows_conv = slot_rows_of(slot_conv, owners, cap_conv, chunks_conv)
    params = small_state[0] * SMALL_SCALE
    seg_ids = segments[0]
    length = seg_ids.shape[0]
    positions = jnp.arange(length)
    causal = (positions[:, None] >= positions[None, :]) & (seg_ids[:, None] == seg_ids[None, :])
    lin_mask = causal.astype(jnp.float32)
    win_mask = (causal & (positions[:, None] - positions[None, :] < WINDOW)).astype(jnp.float32)
    same_prev = [None]
    for shift_by in range(1, TAPS):
        earlier = jnp.pad(seg_ids, (shift_by, 0), constant_values=-1)[:length]
        same_prev.append((earlier == seg_ids).astype(jnp.float32)[:, None])
    column = lax.axis_index("tensor") * half_width
    taps_local = lax.dynamic_slice_in_dim(params[3:], column, half_width, 1)
    x_rows = inputs.astype(jnp.float32)
    normed_one = norm_rows(x_rows, params[0]).astype(jnp.bfloat16)
    conv_in = gather_rows(normed_one)
    value_c = product(conv_in, conv_w[0])
    gate_c = product(conv_in, conv_w[1])
    mixed_c = taps_local[0] * value_c
    for shift_by in range(1, TAPS):
        mixed_c = mixed_c + taps_local[shift_by] * delayed(value_c, shift_by) * same_prev[shift_by]
    gated_conv = (mixed_c * gate_c).astype(jnp.bfloat16)
    hidden_one = x_rows + sum_rows(product(gated_conv, conv_w[2]))
    normed_two = norm_rows(hidden_one, params[1]).astype(jnp.bfloat16)
    mix_in = gather_rows(normed_two)
    projected = [product(mix_in, weight).astype(jnp.bfloat16) for weight in mix_w[:5]]
    query_f = projected[0].reshape(length, local_heads, FEAT)
    key_f = projected[1].reshape(length, local_heads, FEAT)
    query_s = projected[2].reshape(length, local_heads, HEAD)
    key_s = projected[3].reshape(length, local_heads, HEAD)
    values_v = projected[4].reshape(length, local_heads, HEAD)
    _, _, lin_prob, win_prob = attend(query_f, key_f, query_s, key_s, lin_mask, win_mask)
    attended = jnp.einsum(
        "hst,thd->shd", lin_prob.astype(jnp.bfloat16), values_v, preferred_element_type=jnp.float32
    ) + jnp.einsum(
        "hst,thd->shd", win_prob.astype(jnp.bfloat16), values_v, preferred_element_type=jnp.float32
    )
    mix_out = attended.reshape(length, half_width).astype(jnp.bfloat16)
    hidden_two = hidden_one + sum_rows(product(mix_out, mix_w[5]))
    normed_three = norm_rows(hidden_two, params[2]).astype(jnp.bfloat16)
    ff_in = gather_rows(normed_three)
    gate_proj = product(ff_in, mlp_w[0])
    up_proj = product(ff_in, mlp_w[1])
    activated = (jax.nn.silu(gate_proj) * up_proj).astype(jnp.bfloat16)
    result = (hidden_two + sum_rows(product(activated, mlp_w[2]))).astype(jnp.bfloat16)
    back_three = gather_rows(cotangent)
    back_act = product_right(back_three, mlp_w[2])
    gate_sig = jax.nn.sigmoid(gate_proj)
    back_gate = (back_act * up_proj * gate_sig * (1.0 + gate_proj * (1.0 - gate_sig))).astype(
        jnp.bfloat16
    )
    back_up = (back_act * gate_proj * gate_sig).astype(jnp.bfloat16)
    back_normed_three = sum_rows(
        product_right(back_gate, mlp_w[0]) + product_right(back_up, mlp_w[1])
    )
    back_norm_three, gain_three = norm_back(hidden_two, params[2], back_normed_three)
    back_hidden_two = cotangent.astype(jnp.float32) + back_norm_three
    mlp_units = grad_units(None, owners * cap_mlp, rows_mlp, 0, ff_in, back_gate, LANES)
    mlp_units = grad_units(mlp_units, owners * cap_mlp, rows_mlp, wide, ff_in, back_up, LANES)
    mlp_units = grad_units(
        mlp_units, owners * cap_mlp, rows_mlp, 2 * wide, activated, back_three, LANES
    )
    summed_mlp = scatter_sum(mlp_units, owners, cap_mlp, chunks_mlp)
    back_two = gather_rows(back_hidden_two.astype(jnp.bfloat16))
    back_attended = (
        product_right(back_two, mix_w[5]).astype(jnp.bfloat16).reshape(length, local_heads, HEAD)
    )
    lin_again, denom_again, lin_back, win_back = attend(
        query_f, key_f, query_s, key_s, lin_mask, win_mask
    )
    back_prob = jnp.einsum(
        "shd,thd->hst", back_attended, values_v, preferred_element_type=jnp.float32
    )
    back_values = jnp.einsum(
        "hst,shd->thd",
        lin_back.astype(jnp.bfloat16),
        back_attended,
        preferred_element_type=jnp.float32,
    ) + jnp.einsum(
        "hst,shd->thd",
        win_back.astype(jnp.bfloat16),
        back_attended,
        preferred_element_type=jnp.float32,
    )
    back_kernel = (back_prob - jnp.sum(back_prob * lin_back, axis=-1, keepdims=True)) / denom_again
    back_score = (back_kernel * (1.0 + lin_again) * lin_mask).astype(jnp.bfloat16)
    back_query_f = jnp.einsum(
        "hst,thf->shf", back_score, key_f, preferred_element_type=jnp.float32
    ) / math.sqrt(FEAT)
    back_key_f = jnp.einsum(
        "hst,shf->thf", back_score, query_f, preferred_element_type=jnp.float32
    ) / math.sqrt(FEAT)
    back_local = (
        win_back * (back_prob - jnp.sum(back_prob * win_back, axis=-1, keepdims=True))
    ).astype(jnp.bfloat16)
    back_query_s = jnp.einsum(
        "hst,thd->shd", back_local, key_s, preferred_element_type=jnp.float32
    ) / math.sqrt(HEAD)
    back_key_s = jnp.einsum(
        "hst,shd->thd", back_local, query_s, preferred_element_type=jnp.float32
    ) / math.sqrt(HEAD)
    back_projected = [
        piece_grad.reshape(length, -1).astype(jnp.bfloat16)
        for piece_grad in (back_query_f, back_key_f, back_query_s, back_key_s, back_values)
    ]
    back_normed_two = product_right(back_projected[0], mix_w[0])
    for piece_grad, weight in zip(back_projected[1:], mix_w[1:5]):
        back_normed_two = back_normed_two + product_right(piece_grad, weight)
    back_normed_two = sum_rows(back_normed_two)
    back_norm_two, gain_two = norm_back(hidden_one, params[1], back_normed_two)
    back_hidden_one = back_hidden_two + back_norm_two
    mix_rows = owners * cap_mix
    mix_units = None
    unit_at = 0
    for piece_grad in back_projected:
        rows = LANES if piece_grad.shape[1] > LANES else 7 * LANES
        mix_units = grad_units(mix_units, mix_rows, rows_mix, unit_at, mix_in, piece_grad, rows)
        unit_at += per * piece_grad.shape[1] // LANES
    mix_units = grad_units(mix_units, mix_rows, rows_mix, unit_at, mix_out, back_two, LANES)
    summed_mix = scatter_sum(mix_units, owners, cap_mix, chunks_mix)
    back_one = gather_rows(back_hidden_one.astype(jnp.bfloat16))
    back_gated = product_right(back_one, conv_w[2])
    back_mixed = back_gated * gate_c
    back_gate_c = (back_gated * mixed_c).astype(jnp.bfloat16)
    back_value_f = taps_local[0] * back_mixed
    tap_grads = [jnp.sum(back_mixed * value_c, axis=0)]
    for shift_by in range(1, TAPS):
        masked = back_mixed * same_prev[shift_by]
        back_value_f = back_value_f + taps_local[shift_by] * advanced(masked, shift_by)
        tap_grads.append(jnp.sum(masked * delayed(value_c, shift_by), axis=0))
    back_value_c = back_value_f.astype(jnp.bfloat16)
    back_normed_one = sum_rows(
        product_right(back_value_c, conv_w[0]) + product_right(back_gate_c, conv_w[1])
    )
    back_norm_one, gain_one = norm_back(x_rows, params[0], back_normed_one)
    grad_input = back_hidden_one + back_norm_one
    conv_rows = owners * cap_conv
    conv_units = grad_units(None, conv_rows, rows_conv, 0, conv_in, back_value_c, LANES)
    conv_units = grad_units(conv_units, conv_rows, rows_conv, middle, conv_in, back_gate_c, LANES)
    conv_units = grad_units(
        conv_units, conv_rows, rows_conv, 2 * middle, gated_conv, back_one, LANES
    )
    summed_conv = scatter_sum(conv_units, owners, cap_conv, chunks_conv)
    taps_full = lax.dynamic_update_slice(
        jnp.zeros((TAPS, D), jnp.float32), jnp.stack(tap_grads), (jnp.int32(0), column)
    )
    small_grad = jnp.concatenate([jnp.stack([gain_one, gain_two, gain_three]), taps_full], axis=0)
    small_summed = total_of(small_grad, owners)
    new_conv = adam_units(state_conv, summed_conv, slot_conv, CONV_SCALE / owners)
    new_mix = adam_units(state_mix, summed_mix, slot_mix, MIX_SCALE / owners)
    new_mlp = adam_units(state_mlp, summed_mlp, slot_mlp, MLP_SCALE / owners)
    small_new = adam_step(small_state, small_summed * (SMALL_SCALE / owners), SMALL_RATE)
    return (
        result,
        grad_input,
        new_conv,
        new_mix,
        new_mlp,
        small_new[1:],
        small_new[0] - small_state[0],
    )


def solution(mesh):
    placed = (
        P(("dp", "tensor"), None),
        P(("dp", "tensor"), None),
        P("dp", None),
        P(),
        P(),
        P(),
        P(None, "dp", "tensor"),
        P(None, "dp", "tensor"),
        P(None, "dp", "tensor"),
        P(),
    )
    return jax.shard_map(
        per_device,
        mesh=mesh,
        in_specs=placed,
        out_specs=(
            P(("dp", "tensor"), None),
            P(("dp", "tensor"), None),
            P(None, "dp", "tensor"),
            P(None, "dp", "tensor"),
            P(None, "dp", "tensor"),
            P(),
            P(),
        ),
        check_vma=False,
    )
```

```python
import math

import functools

import jax
import jax.numpy as jnp
from jax import lax
from jax.experimental import pallas as pl
from jax.experimental.pallas import tpu as pltpu
from jax.sharding import PartitionSpec as P

MESH = pl.DeviceIdType.MESH
LANES = 128

D = 1792
HEADS = 16
FEAT = 16
FF = 4864
WINDOW = 64
TAPS = 3
STEP = 5
HEAD = 112


NORM_EPS = 1e-05
BETA_ONE = 0.9
BETA_TWO = 0.95
ADAM_EPS = 1e-08
LEARN_RATE = 0.02
SMALL_RATE = 0.16
WEIGHT_DECAY = 0.1
NEG_FILL = -1e30
CONV_SCALE = 0.125
MIX_SCALE = 0.25
MLP_SCALE = 0.5
SMALL_SCALE = 0.125


def norm_rows(values, gain):
    return values * lax.rsqrt(jnp.mean(values * values, axis=-1, keepdims=True) + NORM_EPS) * gain


def norm_back(values, gain, upstream):
    _, pullback = jax.vjp(norm_rows, values, gain)
    return pullback(upstream)


def product(left, right):
    return jnp.dot(left, right, preferred_element_type=jnp.float32)


def product_left(left, right):
    return lax.dot_general(
        left, right, (((0,), (0,)), ((), ())), preferred_element_type=jnp.float32
    )


def product_right(left, right):
    return lax.dot_general(
        left, right, (((1,), (1,)), ((), ())), preferred_element_type=jnp.float32
    )


def swap(values, axis, bit):
    size = lax.axis_size(axis)
    return lax.ppermute(values, axis, [(i, i ^ bit) for i in range(size)])


def gather_rows(piece_rows):
    other = swap(piece_rows, "tensor", 1)
    first = lax.axis_index("tensor") == 0
    return jnp.concatenate(
        [jnp.where(first, piece_rows, other), jnp.where(first, other, piece_rows)]
    )


def sum_rows(piece_rows):
    rows = piece_rows.shape[0] // 2
    at = lax.axis_index("tensor")
    halves = piece_rows.astype(jnp.bfloat16).reshape(2, rows, piece_rows.shape[1])
    other = swap(lax.dynamic_index_in_dim(halves, 1 - at, 0, False), "tensor", 1)
    mine = lax.dynamic_index_in_dim(halves, at, 0, False)
    return mine.astype(jnp.float32) + other.astype(jnp.float32)


def delayed(values, steps):
    return jnp.pad(values, ((steps, 0), (0, 0)))[: values.shape[0]]


def advanced(values, steps):
    return jnp.pad(values, ((0, steps), (0, 0)))[steps:]


def lay_body(first, nu, blocks, m, slots_ref, pooled_ref, out_ref, buf, stage, sem):
    step = pl.program_id(0)
    per_step = nu * blocks

    def fetch(at, half):
        for q in range(per_step):
            pltpu.make_async_copy(
                pooled_ref.at[slots_ref[first + at * per_step + q]], buf.at[half, q], sem.at[half]
            ).start()

    @pl.when(step == 0)
    def _():
        fetch(0, 0)

    @pl.when(step + 1 < pl.num_programs(0))
    def _():
        fetch(step + 1, (step + 1) % 2)

    half = step % 2
    pltpu.make_async_copy(pooled_ref.at[pl.ds(0, per_step)], buf.at[half], sem.at[half]).wait()
    depth = buf.shape[2]
    rows = nu * depth // m
    for block in range(blocks):
        if m == 1:
            for q in range(nu):
                at = (block * nu + q) * depth
                out_ref[at : at + depth, :] = buf[half, block * nu + q]
            continue
        for q in range(nu):
            stage[q * depth : (q + 1) * depth, :] = buf[half, block * nu + q].astype(jnp.float32)
        for c in range(m):
            out_ref[block * rows : (block + 1) * rows, c * LANES : (c + 1) * LANES] = stage[
                pl.ds(c, rows, stride=m), :
            ].astype(jnp.bfloat16)


def lay_out(pooled, slots, first, count, width, nu, blocks):
    depth = pooled.shape[1]
    m = width // LANES
    rows = nu * blocks * depth // m
    steps = count // (nu * blocks)
    assert steps * nu * blocks == count
    return pl.pallas_call(
        functools.partial(lay_body, first, nu, blocks, m),
        grid_spec=pltpu.PrefetchScalarGridSpec(
            num_scalar_prefetch=1,
            grid=(steps,),
            in_specs=[pl.BlockSpec(memory_space=pl.ANY)],
            out_specs=pl.BlockSpec((rows, width), lambda i, s: (i, 0)),
            scratch_shapes=[
                pltpu.VMEM((2, nu * blocks, depth, LANES), jnp.bfloat16),
                pltpu.VMEM((nu * depth, LANES), jnp.float32),
                pltpu.SemaphoreType.DMA((2,)),
            ],
        ),
        out_shape=jax.ShapeDtypeStruct((steps * rows, width), jnp.bfloat16),
        cost_estimate=pl.CostEstimate(
            flops=0, bytes_accessed=4 * count * depth * LANES, transcendentals=0
        ),
        name=f"lay_{width}_{count}",
    )(slots, pooled)


def grad_body(first, nu, m, has_old, slots_ref, u_ref, d_ref, *rest):
    out_ref, stage, buf, sem = rest[1:] if has_old else rest
    step = pl.program_id(0)
    half = step % 2
    depth = buf.shape[2]
    rows = u_ref.shape[1]

    def drain(which):
        pltpu.make_async_copy(out_ref.at[pl.ds(0, nu)], buf.at[which], sem.at[which]).wait()

    @pl.when(step >= 2)
    def _():
        drain(half)

    for c in range(0, m, 2):
        wide = min(2, m - c)
        piece = lax.dot_general(
            u_ref[...],
            d_ref[:, c * LANES : (c + wide) * LANES],
            (((0,), (0,)), ((), ())),
            preferred_element_type=jnp.float32,
        )
        for k in range(wide):
            part = piece[:, k * LANES : (k + 1) * LANES]
            if m == 1:
                stage[...] = part
            else:
                stage[pl.ds(c + k, rows, stride=m), :] = part
    for q in range(nu):
        buf[half, q] = stage[q * depth : (q + 1) * depth, :].astype(jnp.bfloat16)
    for q in range(nu):
        pltpu.make_async_copy(
            buf.at[half, q], out_ref.at[slots_ref[first + step * nu + q]], sem.at[half]
        ).start()

    @pl.when(step + 1 == pl.num_programs(0))
    def _():
        drain(half)

        @pl.when(step >= 1)
        def _():
            drain(1 - half)


def grad_units(old, slot_rows, slots, first, u, d, rows):
    tokens, height = u.shape
    width = d.shape[1]
    m = width // LANES
    depth = LANES
    nu = rows * m // depth
    steps = height // rows
    has_old = old is not None
    shape = jax.ShapeDtypeStruct((slot_rows, depth, LANES), jnp.bfloat16)
    specs = [
        pl.BlockSpec((tokens, rows), lambda i, s: (0, i)),
        pl.BlockSpec((tokens, width), lambda i, s: (0, 0)),
    ]
    operands = [slots, u, d]
    if has_old:
        specs.append(pl.BlockSpec(memory_space=pl.ANY))
        operands.append(old)
    return pl.pallas_call(
        functools.partial(grad_body, first, nu, m, has_old),
        grid_spec=pltpu.PrefetchScalarGridSpec(
            num_scalar_prefetch=1,
            grid=(steps,),
            in_specs=specs,
            out_specs=pl.BlockSpec(memory_space=pl.ANY),
            scratch_shapes=[
                pltpu.VMEM((nu * depth, LANES), jnp.float32),
                pltpu.VMEM((2, nu, depth, LANES), jnp.bfloat16),
                pltpu.SemaphoreType.DMA((2,)),
            ],
        ),
        out_shape=shape,
        input_output_aliases={3: 0} if has_old else {},
        cost_estimate=pl.CostEstimate(
            flops=2 * tokens * height * width,
            bytes_accessed=2 * height * width + 2 * tokens * (height + width),
            transcendentals=0,
        ),
        name=f"grad_{height}_{width}",
    )(*operands)


def bits_of(owners):
    return owners.bit_length() - 1


def chunks_of(total, most):
    number = -(-total // most)
    base, extra = divmod(total, number)
    out, at = [], 0
    for k in range(number):
        size = base + (1 if k < extra else 0)
        out.append((at, size))
        at += size
    return out


def scatter_body(owners, caps, jobs, *refs):
    stages = bits_of(owners)
    groups = len(caps)
    g_refs, out_refs = refs[:groups], refs[groups : 2 * groups]
    landing = [refs[(2 + s) * groups : (3 + s) * groups] for s in range(stages)]
    own, send_sem, recv_sem, own_sem = refs[(2 + stages) * groups :]
    me = lax.axis_index("dp")
    ten = lax.axis_index("tensor")
    bit = [(me // (1 << s)) % 2 for s in range(stages)]
    partner = [me + (1 - 2 * bit[s]) * (1 << s) for s in range(stages)]
    barrier = pltpu.get_barrier_semaphore()
    for s in range(stages):
        pl.semaphore_signal(barrier, inc=1, device_id=(partner[s], ten), device_id_type=MESH)
    pl.semaphore_wait(barrier, stages)
    count = len(jobs)

    def bit_at(s, k):
        if jobs[k][3] and s in (1, 2):
            return 3 - s
        return s

    def sides(s, k):
        before = owners >> s
        inner = 2 if jobs[k][3] and s == 1 else 1
        return before // 2 // inner, inner

    def part(s, k, which):
        g, at, size, _ = jobs[k]
        outer, inner = sides(s, k)
        span = pl.ds(at, size)
        if s == 0:
            return g_refs[g].at[:, which, span]
        ref = landing[s - 1][g]
        view = ref.reshape(outer, 2, inner, *ref.shape[1:])
        return view.at[:, which, :, span]

    def remote(s, k):
        g, at, size, _ = jobs[k]
        outer, inner = sides(s, k)
        span = pl.ds(at, size)
        b = bit_at(s, k)
        ref = landing[s][g]
        dst = ref.at[:, span] if s == 0 else ref.reshape(outer, inner, *ref.shape[1:]).at[:, :, span]
        return pltpu.make_async_remote_copy(
            src_ref=part(s, k, 1 - bit[b]),
            dst_ref=dst,
            send_sem=send_sem.at[s, k],
            recv_sem=recv_sem.at[s, k],
            device_id=(partner[b], ten),
            device_id_type=MESH,
        )

    def local(k):
        return pltpu.make_async_copy(
            part(0, k, bit[0]), own.at[k % 2, :, pl.ds(0, jobs[k][2])], own_sem.at[k % 2]
        )

    for k in range(count):
        remote(0, k).start()
    local(0).start()

    def work(s, k):
        g, at, size, _ = jobs[k]
        left = owners >> (s + 1)
        outer, inner = sides(s, k)
        if s == 0:
            if k + 1 < count:
                local(k + 1).start()
            local(k).wait()
        remote(s, k).wait_recv()
        mine_bit = bit[bit_at(s, k)]
        into = landing[s][g]

        def add(j, carry):
            o, u = j // size, j % size
            if s == 0:
                mine = own[k % 2, o, u]
            else:
                mine = landing[s - 1][g][(o // inner) * 2 * inner + mine_bit * inner + o % inner, at + u]
            total = into[o, at + u].astype(jnp.float32) + mine.astype(jnp.float32)
            if s == stages - 1:
                out_refs[g][at + u] = total
            else:
                into[o, at + u] = total.astype(jnp.bfloat16)
            return carry

        lax.fori_loop(0, left * size, add, 0)
        if s + 1 < stages:
            remote(s + 1, k).start()

    lag = 2
    for t in range(count + lag * (stages - 1)):
        for s in range(stages):
            k = t - lag * s
            if 0 <= k < count:
                work(s, k)
    for s in range(stages):
        for k in range(count):
            remote(s, k).wait_send()


def scatter_sum(units, owners, caps, collective=1, most=6):
    stages = bits_of(owners)
    depth, lanes = units[0].shape[1:]
    jobs = []
    for g, cap in enumerate(caps):
        for at, size in chunks_of(cap, most):
            jobs.append((g, at, size, stages > 2 and len(jobs) % 4 == 2))
    widest = max(size for _, _, size, _ in jobs)
    scratch = []
    for s in range(stages):
        for cap in caps:
            scratch.append(pltpu.VMEM((owners >> (s + 1), cap, depth, lanes), jnp.bfloat16))
    scratch += [
        pltpu.VMEM((2, owners // 2, widest, depth, lanes), jnp.bfloat16),
        pltpu.SemaphoreType.DMA((stages, len(jobs))),
        pltpu.SemaphoreType.DMA((stages, len(jobs))),
        pltpu.SemaphoreType.DMA((2,)),
    ]
    return pl.pallas_call(
        functools.partial(scatter_body, owners, caps, tuple(jobs)),
        out_shape=[jax.ShapeDtypeStruct((cap, depth, lanes), jnp.float32) for cap in caps],
        in_specs=[pl.BlockSpec(memory_space=pl.ANY)] * len(caps),
        out_specs=[pl.BlockSpec(memory_space=pltpu.VMEM)] * len(caps),
        scratch_shapes=scratch,
        compiler_params=pltpu.CompilerParams(collective_id=collective, has_side_effects=True),
        name="scatter_sum",
    )(*[
        group.reshape(owners // 2, 2, cap, depth, lanes) for group, cap in zip(units, caps)
    ])


def total_of(values, owners):
    for b in range(bits_of(owners)):
        values = values + swap(values, "dp", 1 << b)
    return values + swap(values, "tensor", 1)


def adam_values(master, one, two, gradient, rate):
    moment_one = BETA_ONE * one + (1.0 - BETA_ONE) * gradient
    moment_two = BETA_TWO * two + (1.0 - BETA_TWO) * gradient * gradient
    step_size = (
        moment_one
        / (1.0 - BETA_ONE**STEP)
        / (jnp.sqrt(moment_two / (1.0 - BETA_TWO**STEP)) + ADAM_EPS)
    )
    return master - rate * (step_size + WEIGHT_DECAY * master), moment_one, moment_two


def adam_step(opt_state, gradient, rate):
    return jnp.stack(adam_values(opt_state[0], opt_state[1], opt_state[2], gradient, rate))


def adam_body(state_ref, gradient_ref, out_ref):
    new = adam_values(state_ref[0], state_ref[1], state_ref[2], gradient_ref[...], LEARN_RATE)
    for k in range(3):
        out_ref[k] = new[k]


def adam_units(state, summed, slots, scale):
    cap, unit_width = state.shape[1:]
    mine = lax.axis_index("dp") * cap + jnp.arange(cap, dtype=jnp.int32)
    used = jnp.any(mine[:, None] == slots[None, :], axis=1)
    gradient = jnp.where(used[:, None, None], summed * scale, 0.0).reshape(cap, unit_width)
    block = 2048
    return pl.pallas_call(
        adam_body,
        grid=(unit_width // block,),
        in_specs=[
            pl.BlockSpec((3, cap, block), lambda i: (0, 0, i)),
            pl.BlockSpec((cap, block), lambda i: (0, i)),
        ],
        out_specs=pl.BlockSpec((3, cap, block), lambda i: (0, 0, i)),
        out_shape=jax.ShapeDtypeStruct(state.shape, jnp.float32),
        name=f"adam_{cap}",
    )(state, gradient)


def gather_units(state, scale):
    cap, unit_width = state.shape[1:]
    own = (state[0] * scale).reshape(cap, unit_width // LANES, LANES).astype(jnp.bfloat16)
    return lax.all_gather(own, "dp", axis=0, tiled=True)


def attend(query_f, key_f, query_s, key_s, lin_mask, win_mask):
    lin_score = jnp.einsum(
        "shf,thf->hst", query_f, key_f, preferred_element_type=jnp.float32
    ) / math.sqrt(FEAT)
    kernel = (1.0 + lin_score + 0.5 * lin_score * lin_score) * lin_mask
    lin_denom = jnp.sum(kernel, axis=-1, keepdims=True)
    lin_prob = kernel / lin_denom
    win_score = jnp.einsum(
        "shd,thd->hst", query_s, key_s, preferred_element_type=jnp.float32
    ) / math.sqrt(HEAD)
    inside = win_mask > 0
    win_peak = jnp.max(jnp.where(inside, win_score, NEG_FILL), axis=-1, keepdims=True)
    win_exp = jnp.exp(jnp.where(inside, win_score - win_peak, NEG_FILL))
    win_prob = win_exp / jnp.sum(win_exp, axis=-1, keepdims=True)
    return (lin_score, lin_denom, lin_prob, win_prob)


def per_device(
    inputs,
    cotangent,
    segments,
    slot_conv,
    slot_mix,
    slot_mlp,
    state_conv,
    state_mix,
    state_mlp,
    small_state,
):
    tensor_size = lax.axis_size("tensor")
    owners = lax.axis_size("dp")
    half_width = D // tensor_size
    local_heads = HEADS // tensor_size
    feat_cols = local_heads * FEAT
    ff_half = FF // tensor_size
    unit_width = state_conv.shape[2]
    cap_conv = state_conv.shape[1]
    cap_mix = state_mix.shape[1]
    cap_mlp = state_mlp.shape[1]
    pooled = (
        gather_units(state_conv, CONV_SCALE),
        gather_units(state_mix, MIX_SCALE),
        gather_units(state_mlp, MLP_SCALE),
    )
    per = D * LANES // unit_width
    narrow, middle = per * feat_cols // LANES, per * half_width // LANES
    wide = per * ff_half // LANES
    conv_pair = lay_out(pooled[0], slot_conv, 0, 2 * middle, half_width, 7, 2)
    conv_w = [
        conv_pair[:D],
        conv_pair[D:],
        lay_out(pooled[0], slot_conv, 2 * middle, middle, D, 7, 2),
    ]
    feat_pair = lay_out(pooled[1], slot_mix, 0, 2 * narrow, feat_cols, 7, 1)
    mix_trio = lay_out(pooled[1], slot_mix, 2 * narrow, 3 * middle, half_width, 7, 2)
    mix_w = [
        feat_pair[:D],
        feat_pair[D:],
        mix_trio[:D],
        mix_trio[D : 2 * D],
        mix_trio[2 * D :],
        lay_out(pooled[1], slot_mix, 2 * narrow + 3 * middle, middle, D, 7, 2),
    ]
    mlp_pair = lay_out(pooled[2], slot_mlp, 0, 2 * wide, ff_half, 19, 1)
    mlp_w = [
        mlp_pair[:D],
        mlp_pair[D:],
        lay_out(pooled[2], slot_mlp, 2 * wide, wide, D, 7, 2),
    ]
    params = small_state[0] * SMALL_SCALE
    seg_ids = segments[0]
    length = seg_ids.shape[0]
    positions = jnp.arange(length)
    causal = (positions[:, None] >= positions[None, :]) & (seg_ids[:, None] == seg_ids[None, :])
    lin_mask = causal.astype(jnp.float32)
    win_mask = (causal & (positions[:, None] - positions[None, :] < WINDOW)).astype(jnp.float32)
    same_prev = [None]
    for shift_by in range(1, TAPS):
        earlier = jnp.pad(seg_ids, (shift_by, 0), constant_values=-1)[:length]
        same_prev.append((earlier == seg_ids).astype(jnp.float32)[:, None])
    column = lax.axis_index("tensor") * half_width
    taps_local = lax.dynamic_slice_in_dim(params[3:], column, half_width, 1)
    x_rows = inputs.astype(jnp.float32)
    normed_one = norm_rows(x_rows, params[0]).astype(jnp.bfloat16)
    conv_in = gather_rows(normed_one)
    value_c = product(conv_in, conv_w[0])
    gate_c = product(conv_in, conv_w[1])
    mixed_c = taps_local[0] * value_c
    for shift_by in range(1, TAPS):
        mixed_c = mixed_c + taps_local[shift_by] * delayed(value_c, shift_by) * same_prev[shift_by]
    gated_conv = (mixed_c * gate_c).astype(jnp.bfloat16)
    hidden_one = x_rows + sum_rows(product(gated_conv, conv_w[2]))
    normed_two = norm_rows(hidden_one, params[1]).astype(jnp.bfloat16)
    mix_in = gather_rows(normed_two)
    projected = [product(mix_in, weight).astype(jnp.bfloat16) for weight in mix_w[:5]]
    query_f = projected[0].reshape(length, local_heads, FEAT)
    key_f = projected[1].reshape(length, local_heads, FEAT)
    query_s = projected[2].reshape(length, local_heads, HEAD)
    key_s = projected[3].reshape(length, local_heads, HEAD)
    values_v = projected[4].reshape(length, local_heads, HEAD)
    _, _, lin_prob, win_prob = attend(query_f, key_f, query_s, key_s, lin_mask, win_mask)
    attended = jnp.einsum(
        "hst,thd->shd", lin_prob.astype(jnp.bfloat16), values_v, preferred_element_type=jnp.float32
    ) + jnp.einsum(
        "hst,thd->shd", win_prob.astype(jnp.bfloat16), values_v, preferred_element_type=jnp.float32
    )
    mix_out = attended.reshape(length, half_width).astype(jnp.bfloat16)
    hidden_two = hidden_one + sum_rows(product(mix_out, mix_w[5]))
    normed_three = norm_rows(hidden_two, params[2]).astype(jnp.bfloat16)
    ff_in = gather_rows(normed_three)
    gate_proj = product(ff_in, mlp_w[0])
    up_proj = product(ff_in, mlp_w[1])
    activated = (jax.nn.silu(gate_proj) * up_proj).astype(jnp.bfloat16)
    result = (hidden_two + sum_rows(product(activated, mlp_w[2]))).astype(jnp.bfloat16)
    back_three = gather_rows(cotangent)
    back_act = product_right(back_three, mlp_w[2])
    gate_sig = jax.nn.sigmoid(gate_proj)
    back_gate = (back_act * up_proj * gate_sig * (1.0 + gate_proj * (1.0 - gate_sig))).astype(
        jnp.bfloat16
    )
    back_up = (back_act * gate_proj * gate_sig).astype(jnp.bfloat16)
    back_normed_three = sum_rows(
        product_right(back_gate, mlp_w[0]) + product_right(back_up, mlp_w[1])
    )
    back_norm_three, gain_three = norm_back(hidden_two, params[2], back_normed_three)
    back_hidden_two = cotangent.astype(jnp.float32) + back_norm_three
    mlp_units = grad_units(None, owners * cap_mlp, slot_mlp, 0, ff_in, back_gate, LANES)
    mlp_units = grad_units(mlp_units, owners * cap_mlp, slot_mlp, wide, ff_in, back_up, LANES)
    mlp_units = grad_units(
        mlp_units, owners * cap_mlp, slot_mlp, 2 * wide, activated, back_three, LANES
    )
    summed_mlp = lax.psum_scatter(
        mlp_units, "dp", scatter_dimension=0, tiled=True
    ).astype(jnp.float32)
    back_two = gather_rows(back_hidden_two.astype(jnp.bfloat16))
    back_attended = (
        product_right(back_two, mix_w[5]).astype(jnp.bfloat16).reshape(length, local_heads, HEAD)
    )
    lin_again, denom_again, lin_back, win_back = attend(
        query_f, key_f, query_s, key_s, lin_mask, win_mask
    )
    back_prob = jnp.einsum(
        "shd,thd->hst", back_attended, values_v, preferred_element_type=jnp.float32
    )
    back_values = jnp.einsum(
        "hst,shd->thd",
        lin_back.astype(jnp.bfloat16),
        back_attended,
        preferred_element_type=jnp.float32,
    ) + jnp.einsum(
        "hst,shd->thd",
        win_back.astype(jnp.bfloat16),
        back_attended,
        preferred_element_type=jnp.float32,
    )
    back_kernel = (back_prob - jnp.sum(back_prob * lin_back, axis=-1, keepdims=True)) / denom_again
    back_score = (back_kernel * (1.0 + lin_again) * lin_mask).astype(jnp.bfloat16)
    back_query_f = jnp.einsum(
        "hst,thf->shf", back_score, key_f, preferred_element_type=jnp.float32
    ) / math.sqrt(FEAT)
    back_key_f = jnp.einsum(
        "hst,shf->thf", back_score, query_f, preferred_element_type=jnp.float32
    ) / math.sqrt(FEAT)
    back_local = (
        win_back * (back_prob - jnp.sum(back_prob * win_back, axis=-1, keepdims=True))
    ).astype(jnp.bfloat16)
    back_query_s = jnp.einsum(
        "hst,thd->shd", back_local, key_s, preferred_element_type=jnp.float32
    ) / math.sqrt(HEAD)
    back_key_s = jnp.einsum(
        "hst,shd->thd", back_local, query_s, preferred_element_type=jnp.float32
    ) / math.sqrt(HEAD)
    back_projected = [
        piece_grad.reshape(length, -1).astype(jnp.bfloat16)
        for piece_grad in (back_query_f, back_key_f, back_query_s, back_key_s, back_values)
    ]
    back_normed_two = product_right(back_projected[0], mix_w[0])
    for piece_grad, weight in zip(back_projected[1:], mix_w[1:5]):
        back_normed_two = back_normed_two + product_right(piece_grad, weight)
    back_normed_two = sum_rows(back_normed_two)
    back_norm_two, gain_two = norm_back(hidden_one, params[1], back_normed_two)
    back_hidden_one = back_hidden_two + back_norm_two
    mix_rows = owners * cap_mix
    mix_units = None
    unit_at = 0
    for piece_grad in back_projected:
        rows = LANES if piece_grad.shape[1] > LANES else 7 * LANES
        mix_units = grad_units(mix_units, mix_rows, slot_mix, unit_at, mix_in, piece_grad, rows)
        unit_at += per * piece_grad.shape[1] // LANES
    mix_units = grad_units(mix_units, mix_rows, slot_mix, unit_at, mix_out, back_two, LANES)
    back_one = gather_rows(back_hidden_one.astype(jnp.bfloat16))
    back_gated = product_right(back_one, conv_w[2])
    back_mixed = back_gated * gate_c
    back_gate_c = (back_gated * mixed_c).astype(jnp.bfloat16)
    back_value_f = taps_local[0] * back_mixed
    tap_grads = [jnp.sum(back_mixed * value_c, axis=0)]
    for shift_by in range(1, TAPS):
        masked = back_mixed * same_prev[shift_by]
        back_value_f = back_value_f + taps_local[shift_by] * advanced(masked, shift_by)
        tap_grads.append(jnp.sum(masked * delayed(value_c, shift_by), axis=0))
    back_value_c = back_value_f.astype(jnp.bfloat16)
    back_normed_one = sum_rows(
        product_right(back_value_c, conv_w[0]) + product_right(back_gate_c, conv_w[1])
    )
    back_norm_one, gain_one = norm_back(x_rows, params[0], back_normed_one)
    grad_input = back_hidden_one + back_norm_one
    conv_rows = owners * cap_conv
    conv_units = grad_units(None, conv_rows, slot_conv, 0, conv_in, back_value_c, LANES)
    conv_units = grad_units(conv_units, conv_rows, slot_conv, middle, conv_in, back_gate_c, LANES)
    conv_units = grad_units(
        conv_units, conv_rows, slot_conv, 2 * middle, gated_conv, back_one, LANES
    )
    summed_mix, summed_conv = scatter_sum((mix_units, conv_units), owners, (cap_mix, cap_conv))
    taps_full = lax.dynamic_update_slice(
        jnp.zeros((TAPS, D), jnp.float32), jnp.stack(tap_grads), (jnp.int32(0), column)
    )
    small_grad = jnp.concatenate([jnp.stack([gain_one, gain_two, gain_three]), taps_full], axis=0)
    small_summed = total_of(small_grad, owners)
    new_conv = adam_units(state_conv, summed_conv, slot_conv, CONV_SCALE / owners)
    new_mix = adam_units(state_mix, summed_mix, slot_mix, MIX_SCALE / owners)
    new_mlp = adam_units(state_mlp, summed_mlp, slot_mlp, MLP_SCALE / owners)
    small_new = adam_step(small_state, small_summed * (SMALL_SCALE / owners), SMALL_RATE)
    return (
        result,
        grad_input,
        new_conv,
        new_mix,
        new_mlp,
        small_new[1:],
        small_new[0] - small_state[0],
    )


def solution(mesh):
    placed = (
        P(("dp", "tensor"), None),
        P(("dp", "tensor"), None),
        P("dp", None),
        P(),
        P(),
        P(),
        P(None, "dp", "tensor"),
        P(None, "dp", "tensor"),
        P(None, "dp", "tensor"),
        P(),
    )
    return jax.shard_map(
        per_device,
        mesh=mesh,
        in_specs=placed,
        out_specs=(
            P(("dp", "tensor"), None),
            P(("dp", "tensor"), None),
            P(None, "dp", "tensor"),
            P(None, "dp", "tensor"),
            P(None, "dp", "tensor"),
            P(),
            P(),
        ),
        check_vma=False,
    )
```

```python
import math

import functools

import jax
import jax.numpy as jnp
from jax import lax
from jax.experimental import pallas as pl
from jax.experimental.pallas import tpu as pltpu
from jax.sharding import PartitionSpec as P

MESH = pl.DeviceIdType.MESH
LANES = 128

D = 1792
HEADS = 16
FEAT = 16
FF = 4864
WINDOW = 64
TAPS = 3
STEP = 5
HEAD = 112


NORM_EPS = 1e-05
BETA_ONE = 0.9
BETA_TWO = 0.95
ADAM_EPS = 1e-08
LEARN_RATE = 0.02
SMALL_RATE = 0.16
WEIGHT_DECAY = 0.1
NEG_FILL = -1e30
CONV_SCALE = 0.125
MIX_SCALE = 0.25
MLP_SCALE = 0.5
SMALL_SCALE = 0.125


def norm_rows(values, gain):
    return values * lax.rsqrt(jnp.mean(values * values, axis=-1, keepdims=True) + NORM_EPS) * gain


def norm_back(values, gain, upstream):
    _, pullback = jax.vjp(norm_rows, values, gain)
    return pullback(upstream)


def product(left, right):
    return jnp.dot(left, right, preferred_element_type=jnp.float32)


def product_left(left, right):
    return lax.dot_general(
        left, right, (((0,), (0,)), ((), ())), preferred_element_type=jnp.float32
    )


def product_right(left, right):
    return lax.dot_general(
        left, right, (((1,), (1,)), ((), ())), preferred_element_type=jnp.float32
    )


def swap(values, axis, bit):
    size = lax.axis_size(axis)
    return lax.ppermute(values, axis, [(i, i ^ bit) for i in range(size)])


def gather_rows(piece_rows):
    other = swap(piece_rows, "tensor", 1)
    first = lax.axis_index("tensor") == 0
    return jnp.concatenate(
        [jnp.where(first, piece_rows, other), jnp.where(first, other, piece_rows)]
    )


def sum_rows(piece_rows):
    rows = piece_rows.shape[0] // 2
    at = lax.axis_index("tensor")
    halves = piece_rows.astype(jnp.bfloat16).reshape(2, rows, piece_rows.shape[1])
    other = swap(lax.dynamic_index_in_dim(halves, 1 - at, 0, False), "tensor", 1)
    mine = lax.dynamic_index_in_dim(halves, at, 0, False)
    return mine.astype(jnp.float32) + other.astype(jnp.float32)


def delayed(values, steps):
    return jnp.pad(values, ((steps, 0), (0, 0)))[: values.shape[0]]


def advanced(values, steps):
    return jnp.pad(values, ((0, steps), (0, 0)))[steps:]


def lay_body(parts, slots_ref, pooled_ref, *refs):
    out_refs, (buf, stage, sem) = refs[: len(parts)], refs[len(parts) :]
    step = pl.program_id(0)
    depth = buf.shape[2]
    starts = [sum(part[4] for part in parts[:p]) for p in range(len(parts))]

    def inside(at, p):
        return (at >= starts[p]) & (at < starts[p] + parts[p][4])

    def fetch(at, half):
        for p, (first, nu, blocks, _, _) in enumerate(parts):

            @pl.when(inside(at, p))
            def _():
                for q in range(nu * blocks):
                    unit = first + (at - starts[p]) * (nu * blocks) + q
                    pltpu.make_async_copy(
                        pooled_ref.at[slots_ref[unit]], buf.at[half, q], sem.at[half]
                    ).start()

    @pl.when(step == 0)
    def _():
        fetch(0, 0)

    @pl.when(step + 1 < pl.num_programs(0))
    def _():
        fetch(step + 1, (step + 1) % 2)

    half = step % 2
    for p, (first, nu, blocks, m, _) in enumerate(parts):
        out_ref = out_refs[p]
        rows = nu * depth // m

        @pl.when(inside(step, p))
        def _():
            pltpu.make_async_copy(
                pooled_ref.at[pl.ds(0, nu * blocks)], buf.at[half, pl.ds(0, nu * blocks)], sem.at[half]
            ).wait()
            for block in range(blocks):
                if m == 1:
                    for q in range(nu):
                        at = (block * nu + q) * depth
                        out_ref[at : at + depth, :] = buf[half, block * nu + q]
                    continue
                base = (block % 2) * stage.shape[0] // 2
                for q in range(nu):
                    at = base + q * depth
                    stage[at : at + depth, :] = buf[half, block * nu + q].astype(jnp.float32)
                for c in range(m):
                    out_ref[block * rows : (block + 1) * rows, c * LANES : (c + 1) * LANES] = stage[
                        pl.ds(base + c, rows, stride=m), :
                    ].astype(jnp.bfloat16)


def lay_out(pooled, slots, wanted):
    depth = pooled.shape[1]
    parts, specs, shapes = [], [], []
    first = start = 0
    for count, width, nu, blocks in wanted:
        m = width // LANES
        steps = count // (nu * blocks)
        rows = nu * blocks * depth // m
        assert steps * nu * blocks == count
        parts.append((first, nu, blocks, m, steps))

        def place(i, s, start=start, steps=steps):
            return (jnp.clip(i - start, 0, steps - 1), 0)

        specs.append(pl.BlockSpec((rows, width), place))
        shapes.append(jax.ShapeDtypeStruct((steps * rows, width), jnp.bfloat16))
        first += count
        start += steps
    return pl.pallas_call(
        functools.partial(lay_body, tuple(parts)),
        grid_spec=pltpu.PrefetchScalarGridSpec(
            num_scalar_prefetch=1,
            grid=(start,),
            in_specs=[pl.BlockSpec(memory_space=pl.ANY)],
            out_specs=specs,
            scratch_shapes=[
                pltpu.VMEM((2, max(p[1] * p[2] for p in parts), depth, LANES), jnp.bfloat16),
                pltpu.VMEM((2 * max(p[1] for p in parts) * depth, LANES), jnp.float32),
                pltpu.SemaphoreType.DMA((2,)),
            ],
        ),
        out_shape=shapes,
        cost_estimate=pl.CostEstimate(
            flops=0, bytes_accessed=4 * first * depth * LANES, transcendentals=0
        ),
        name=f"lay_{first}",
    )(slots, pooled)


def grad_body(parts, sources, slots_ref, *refs):
    ins, out_ref, stage = refs[:sources], refs[sources], refs[sources + 1]
    bufs, sem = refs[sources + 2 : -1], refs[-1]
    depth = LANES

    def drain(p, half):
        nu = bufs[p].shape[1]
        pltpu.make_async_copy(out_ref.at[pl.ds(0, nu)], bufs[p].at[half], sem.at[p, half]).wait()

    for p, (first, rows, left, right) in enumerate(parts):
        u_ref, d_ref, buf = ins[left], ins[right], bufs[p]
        m = d_ref.shape[1] // LANES
        nu = rows * m // depth

        def step_of(step, carry):
            half = step % 2

            @pl.when(step >= 2)
            def _():
                drain(p, half)

            at = pl.multiple_of(step * rows, LANES)
            turned = u_ref[:, pl.ds(at, rows)].T
            for c in range(0, m, 2):
                wide = min(2, m - c)
                piece = jnp.dot(
                    turned,
                    d_ref[:, c * LANES : (c + wide) * LANES],
                    preferred_element_type=jnp.float32,
                )
                for k in range(wide):
                    part = piece[:, k * LANES : (k + 1) * LANES]
                    if m == 1:
                        stage[:rows, :] = part
                    else:
                        stage[pl.ds(c + k, rows, stride=m), :] = part
            for q in range(nu):
                buf[half, q] = stage[q * depth : (q + 1) * depth, :].astype(jnp.bfloat16)
            for q in range(nu):
                pltpu.make_async_copy(
                    buf.at[half, q], out_ref.at[slots_ref[first + step * nu + q]], sem.at[p, half]
                ).start()
            return carry

        lax.fori_loop(0, u_ref.shape[1] // rows, step_of, 0)
    for p, (first, rows, left, right) in enumerate(parts):
        steps = ins[left].shape[1] // rows
        drain(p, (steps - 1) % 2)
        if steps > 1:
            drain(p, steps % 2)


def grad_units(slot_rows, slots, wanted):
    operands, parts, bufs = [], [], []
    first = most = flops = 0
    where = {}
    for u, d, rows in wanted:
        for value in (u, d):
            if id(value) not in where:
                where[id(value)] = len(operands)
                operands.append(value)
        height, width = u.shape[1], d.shape[1]
        nu = rows * width // LANES // LANES
        parts.append((first, rows, where[id(u)], where[id(d)]))
        bufs.append(pltpu.VMEM((2, nu, LANES, LANES), jnp.bfloat16))
        first += height * width // LANES // LANES
        most = max(most, nu)
        flops += 2 * u.shape[0] * height * width
    return pl.pallas_call(
        functools.partial(grad_body, tuple(parts), len(operands)),
        grid_spec=pltpu.PrefetchScalarGridSpec(
            num_scalar_prefetch=1,
            in_specs=[pl.BlockSpec(memory_space=pltpu.VMEM)] * len(operands),
            out_specs=pl.BlockSpec(memory_space=pl.ANY),
            scratch_shapes=[
                pltpu.VMEM((most * LANES, LANES), jnp.float32),
                *bufs,
                pltpu.SemaphoreType.DMA((len(parts), 2)),
            ],
        ),
        out_shape=jax.ShapeDtypeStruct((slot_rows, LANES, LANES), jnp.bfloat16),
        cost_estimate=pl.CostEstimate(
            flops=flops, bytes_accessed=2 * first * LANES * LANES, transcendentals=0
        ),
        name=f"grad_{first}",
    )(slots, *operands)


def bits_of(owners):
    return owners.bit_length() - 1


def chunks_of(total, most):
    number = -(-total // most)
    base, extra = divmod(total, number)
    out, at = [], 0
    for k in range(number):
        size = base + (1 if k < extra else 0)
        out.append((at, size))
        at += size
    return out


def scatter_body(owners, caps, jobs, *refs):
    stages = bits_of(owners)
    groups = len(caps)
    g_refs, small_ref = refs[:groups], refs[groups]
    out_refs, small_out = refs[groups + 1 : 2 * groups + 1], refs[2 * groups + 1]
    refs = refs[2 * groups + 2 :]
    landing = [refs[s * groups : (s + 1) * groups] for s in range(stages)]
    own, small_sum, small_land, send_sem, recv_sem, own_sem, small_send, small_recv = refs[
        stages * groups :
    ]
    me = lax.axis_index("dp")
    ten = lax.axis_index("tensor")
    bit = [(me // (1 << s)) % 2 for s in range(stages)]
    partner = [me + (1 - 2 * bit[s]) * (1 << s) for s in range(stages)]
    barrier = pltpu.get_barrier_semaphore()
    for s in range(stages):
        pl.semaphore_signal(barrier, inc=1, device_id=(partner[s], ten), device_id_type=MESH)
    pl.semaphore_signal(barrier, inc=1, device_id=(me, 1 - ten), device_id_type=MESH)
    pl.semaphore_wait(barrier, stages + 1)
    count = len(jobs)

    def small(s):
        to = (me, 1 - ten) if s == stages else (partner[s], ten)
        return pltpu.make_async_remote_copy(
            src_ref=small_ref if s == 0 else small_sum.at[s - 1],
            dst_ref=small_land.at[s],
            send_sem=small_send.at[s],
            recv_sem=small_recv.at[s],
            device_id=to,
            device_id_type=MESH,
        )

    def small_step(s):
        small(s).wait_recv()
        total = (small_ref[...] if s == 0 else small_sum[s - 1]) + small_land[s]
        if s == stages:
            small_out[...] = total
        else:
            small_sum[s] = total
            small(s + 1).start()

    small(0).start()

    def bit_at(s, k):
        if jobs[k][3] and s in (1, 2):
            return 3 - s
        return s

    def sides(s, k):
        before = owners >> s
        inner = 2 if jobs[k][3] and s == 1 else 1
        return before // 2 // inner, inner

    def part(s, k, which):
        g, at, size, _ = jobs[k]
        outer, inner = sides(s, k)
        span = pl.ds(at, size)
        if s == 0:
            return g_refs[g].at[:, which, span]
        ref = landing[s - 1][g]
        view = ref.reshape(outer, 2, inner, *ref.shape[1:])
        return view.at[:, which, :, span]

    def remote(s, k):
        g, at, size, _ = jobs[k]
        outer, inner = sides(s, k)
        span = pl.ds(at, size)
        b = bit_at(s, k)
        ref = landing[s][g]
        dst = ref.at[:, span] if s == 0 else ref.reshape(outer, inner, *ref.shape[1:]).at[:, :, span]
        return pltpu.make_async_remote_copy(
            src_ref=part(s, k, 1 - bit[b]),
            dst_ref=dst,
            send_sem=send_sem.at[s, k],
            recv_sem=recv_sem.at[s, k],
            device_id=(partner[b], ten),
            device_id_type=MESH,
        )

    def local(k):
        return pltpu.make_async_copy(
            part(0, k, bit[0]), own.at[k % 2, :, pl.ds(0, jobs[k][2])], own_sem.at[k % 2]
        )

    for k in range(count):
        remote(0, k).start()
    local(0).start()

    def work(s, k):
        g, at, size, _ = jobs[k]
        left = owners >> (s + 1)
        outer, inner = sides(s, k)
        if s == 0:
            if k + 1 < count:
                local(k + 1).start()
            local(k).wait()
        remote(s, k).wait_recv()
        mine_bit = bit[bit_at(s, k)]
        into = landing[s][g]

        def add(j, carry):
            o, u = j // size, j % size
            if s == 0:
                mine = own[k % 2, o, u]
            else:
                mine = landing[s - 1][g][(o // inner) * 2 * inner + mine_bit * inner + o % inner, at + u]
            total = into[o, at + u].astype(jnp.float32) + mine.astype(jnp.float32)
            if s == stages - 1:
                out_refs[g][at + u] = total
            else:
                into[o, at + u] = total.astype(jnp.bfloat16)
            return carry

        lax.fori_loop(0, left * size, add, 0)
        if s + 1 < stages:
            remote(s + 1, k).start()

    lag = 2
    for t in range(count + lag * (stages - 1)):
        for s in range(stages):
            k = t - lag * s
            if 0 <= k < count:
                work(s, k)
        if t % 2 == 1 and t // 2 <= stages:
            small_step(t // 2)
    for s in range(stages):
        for k in range(count):
            remote(s, k).wait_send()
    for s in range(stages + 1):
        small(s).wait_send()


def scatter_sum(units, small, owners, caps, collective=1, most=4):
    stages = bits_of(owners)
    depth, lanes = units[0].shape[1:]
    jobs = []
    for g, cap in enumerate(caps):
        for at, size in chunks_of(cap, most):
            jobs.append((g, at, size, stages > 2 and len(jobs) % 4 == 2))
    widest = max(size for _, _, size, _ in jobs)
    assert len(jobs) + 2 * (stages - 1) > 2 * stages + 1
    scratch = []
    for s in range(stages):
        for cap in caps:
            scratch.append(pltpu.VMEM((owners >> (s + 1), cap, depth, lanes), jnp.bfloat16))
    scratch += [
        pltpu.VMEM((2, owners // 2, widest, depth, lanes), jnp.bfloat16),
        pltpu.VMEM((stages, *small.shape), jnp.float32),
        pltpu.VMEM((stages + 1, *small.shape), jnp.float32),
        pltpu.SemaphoreType.DMA((stages, len(jobs))),
        pltpu.SemaphoreType.DMA((stages, len(jobs))),
        pltpu.SemaphoreType.DMA((2,)),
        pltpu.SemaphoreType.DMA((stages + 1,)),
        pltpu.SemaphoreType.DMA((stages + 1,)),
    ]
    return pl.pallas_call(
        functools.partial(scatter_body, owners, caps, tuple(jobs)),
        out_shape=[
            *[jax.ShapeDtypeStruct((cap, depth, lanes), jnp.float32) for cap in caps],
            jax.ShapeDtypeStruct(small.shape, jnp.float32),
        ],
        in_specs=[
            *[pl.BlockSpec(memory_space=pl.ANY)] * len(caps),
            pl.BlockSpec(memory_space=pltpu.VMEM),
        ],
        out_specs=[pl.BlockSpec(memory_space=pltpu.VMEM)] * (len(caps) + 1),
        scratch_shapes=scratch,
        compiler_params=pltpu.CompilerParams(collective_id=collective, has_side_effects=True),
        name="scatter_sum",
    )(
        *[group.reshape(owners // 2, 2, cap, depth, lanes) for group, cap in zip(units, caps)],
        small,
    )


def adam_values(master, one, two, gradient, rate):
    moment_one = BETA_ONE * one + (1.0 - BETA_ONE) * gradient
    moment_two = BETA_TWO * two + (1.0 - BETA_TWO) * gradient * gradient
    step_size = (
        moment_one
        / (1.0 - BETA_ONE**STEP)
        / (jnp.sqrt(moment_two / (1.0 - BETA_TWO**STEP)) + ADAM_EPS)
    )
    return master - rate * (step_size + WEIGHT_DECAY * master), moment_one, moment_two


def adam_step(opt_state, gradient, rate):
    return jnp.stack(adam_values(opt_state[0], opt_state[1], opt_state[2], gradient, rate))


def adam_body(scale, used_ref, state_ref, summed_ref, out_ref):
    cap, rows, lanes = summed_ref.shape
    flat = summed_ref.reshape(cap * rows, lanes)
    used = used_ref[...] > 0
    for r in range(rows):
        here = slice(r * lanes, (r + 1) * lanes)
        summed = flat[pl.ds(r, cap, stride=rows), :] * scale
        gradient = jnp.where(used, summed, 0.0)
        new = adam_values(
            state_ref[0, :, here], state_ref[1, :, here], state_ref[2, :, here], gradient, LEARN_RATE
        )
        for k in range(3):
            out_ref[k, :, here] = new[k]


def adam_units(state, summed, slots, scale):
    cap, unit_width = state.shape[1:]
    mine = lax.axis_index("dp") * cap + jnp.arange(cap, dtype=jnp.int32)
    used = jnp.any(mine[:, None] == slots[None, :], axis=1).astype(jnp.int32)
    rows = 16
    block = rows * LANES
    return pl.pallas_call(
        functools.partial(adam_body, scale),
        grid=(unit_width // block,),
        in_specs=[
            pl.BlockSpec((cap, LANES), lambda i: (0, 0)),
            pl.BlockSpec((3, cap, block), lambda i: (0, 0, i)),
            pl.BlockSpec((cap, rows, LANES), lambda i: (0, i, 0)),
        ],
        out_specs=pl.BlockSpec((3, cap, block), lambda i: (0, 0, i)),
        out_shape=jax.ShapeDtypeStruct(state.shape, jnp.float32),
        name=f"adam_{cap}",
    )(jnp.broadcast_to(used[:, None], (cap, LANES)), state, summed)


def gather_units(state, scale):
    cap, unit_width = state.shape[1:]
    own = (state[0] * scale).reshape(cap, unit_width // LANES, LANES).astype(jnp.bfloat16)
    return lax.all_gather(own, "dp", axis=0, tiled=True)


def attend(query_f, key_f, query_s, key_s, lin_mask, win_mask):
    lin_score = jnp.einsum(
        "shf,thf->hst", query_f, key_f, preferred_element_type=jnp.float32
    ) / math.sqrt(FEAT)
    kernel = (1.0 + lin_score + 0.5 * lin_score * lin_score) * lin_mask
    lin_denom = jnp.sum(kernel, axis=-1, keepdims=True)
    lin_prob = kernel / lin_denom
    win_score = jnp.einsum(
        "shd,thd->hst", query_s, key_s, preferred_element_type=jnp.float32
    ) / math.sqrt(HEAD)
    inside = win_mask > 0
    win_peak = jnp.max(jnp.where(inside, win_score, NEG_FILL), axis=-1, keepdims=True)
    win_exp = jnp.exp(jnp.where(inside, win_score - win_peak, NEG_FILL))
    win_prob = win_exp / jnp.sum(win_exp, axis=-1, keepdims=True)
    return (lin_score, lin_denom, lin_prob, win_prob)


def per_device(
    inputs,
    cotangent,
    segments,
    slot_conv,
    slot_mix,
    slot_mlp,
    state_conv,
    state_mix,
    state_mlp,
    small_state,
):
    tensor_size = lax.axis_size("tensor")
    owners = lax.axis_size("dp")
    half_width = D // tensor_size
    local_heads = HEADS // tensor_size
    feat_cols = local_heads * FEAT
    ff_half = FF // tensor_size
    unit_width = state_conv.shape[2]
    cap_conv = state_conv.shape[1]
    cap_mix = state_mix.shape[1]
    cap_mlp = state_mlp.shape[1]
    pooled = (
        gather_units(state_conv, CONV_SCALE),
        gather_units(state_mix, MIX_SCALE),
        gather_units(state_mlp, MLP_SCALE),
    )
    per = D * LANES // unit_width
    narrow, middle = per * feat_cols // LANES, per * half_width // LANES
    wide = per * ff_half // LANES
    conv_pair, conv_back = lay_out(
        pooled[0], slot_conv, ((2 * middle, half_width, 7, 2), (middle, D, 7, 2))
    )
    conv_w = [conv_pair[:D], conv_pair[D:], conv_back]
    feat_pair, mix_trio, mix_back = lay_out(
        pooled[1],
        slot_mix,
        ((2 * narrow, feat_cols, 7, 2), (3 * middle, half_width, 7, 3), (middle, D, 7, 2)),
    )
    mix_w = [
        feat_pair[:D],
        feat_pair[D:],
        mix_trio[:D],
        mix_trio[D : 2 * D],
        mix_trio[2 * D :],
        mix_back,
    ]
    mlp_pair, mlp_back = lay_out(
        pooled[2], slot_mlp, ((2 * wide, ff_half, 19, 2), (wide, D, 7, 2))
    )
    mlp_w = [mlp_pair[:D], mlp_pair[D:], mlp_back]
    params = small_state[0] * SMALL_SCALE
    seg_ids = segments[0]
    length = seg_ids.shape[0]
    positions = jnp.arange(length)
    causal = (positions[:, None] >= positions[None, :]) & (seg_ids[:, None] == seg_ids[None, :])
    lin_mask = causal.astype(jnp.float32)
    win_mask = (causal & (positions[:, None] - positions[None, :] < WINDOW)).astype(jnp.float32)
    same_prev = [None]
    for shift_by in range(1, TAPS):
        earlier = jnp.pad(seg_ids, (shift_by, 0), constant_values=-1)[:length]
        same_prev.append((earlier == seg_ids).astype(jnp.float32)[:, None])
    column = lax.axis_index("tensor") * half_width
    taps_local = lax.dynamic_slice_in_dim(params[3:], column, half_width, 1)
    x_rows = inputs.astype(jnp.float32)
    normed_one = norm_rows(x_rows, params[0]).astype(jnp.bfloat16)
    conv_in = gather_rows(normed_one)
    value_c = product(conv_in, conv_w[0])
    gate_c = product(conv_in, conv_w[1])
    mixed_c = taps_local[0] * value_c
    for shift_by in range(1, TAPS):
        mixed_c = mixed_c + taps_local[shift_by] * delayed(value_c, shift_by) * same_prev[shift_by]
    gated_conv = (mixed_c * gate_c).astype(jnp.bfloat16)
    hidden_one = x_rows + sum_rows(product(gated_conv, conv_w[2]))
    normed_two = norm_rows(hidden_one, params[1]).astype(jnp.bfloat16)
    mix_in = gather_rows(normed_two)
    projected = [product(mix_in, weight).astype(jnp.bfloat16) for weight in mix_w[:5]]
    query_f = projected[0].reshape(length, local_heads, FEAT)
    key_f = projected[1].reshape(length, local_heads, FEAT)
    query_s = projected[2].reshape(length, local_heads, HEAD)
    key_s = projected[3].reshape(length, local_heads, HEAD)
    values_v = projected[4].reshape(length, local_heads, HEAD)
    _, _, lin_prob, win_prob = attend(query_f, key_f, query_s, key_s, lin_mask, win_mask)
    attended = jnp.einsum(
        "hst,thd->shd", lin_prob.astype(jnp.bfloat16), values_v, preferred_element_type=jnp.float32
    ) + jnp.einsum(
        "hst,thd->shd", win_prob.astype(jnp.bfloat16), values_v, preferred_element_type=jnp.float32
    )
    mix_out = attended.reshape(length, half_width).astype(jnp.bfloat16)
    hidden_two = hidden_one + sum_rows(product(mix_out, mix_w[5]))
    normed_three = norm_rows(hidden_two, params[2]).astype(jnp.bfloat16)
    ff_in = gather_rows(normed_three)
    gate_proj = product(ff_in, mlp_w[0])
    up_proj = product(ff_in, mlp_w[1])
    activated = (jax.nn.silu(gate_proj) * up_proj).astype(jnp.bfloat16)
    result = (hidden_two + sum_rows(product(activated, mlp_w[2]))).astype(jnp.bfloat16)
    back_three = gather_rows(cotangent)
    back_act = product_right(back_three, mlp_w[2])
    gate_sig = jax.nn.sigmoid(gate_proj)
    back_gate = (back_act * up_proj * gate_sig * (1.0 + gate_proj * (1.0 - gate_sig))).astype(
        jnp.bfloat16
    )
    back_up = (back_act * gate_proj * gate_sig).astype(jnp.bfloat16)
    back_normed_three = sum_rows(
        product_right(back_gate, mlp_w[0]) + product_right(back_up, mlp_w[1])
    )
    back_norm_three, gain_three = norm_back(hidden_two, params[2], back_normed_three)
    back_hidden_two = cotangent.astype(jnp.float32) + back_norm_three
    mlp_units = grad_units(
        owners * cap_mlp,
        slot_mlp,
        (
            (ff_in, back_gate, 2 * LANES),
            (ff_in, back_up, 2 * LANES),
            (activated, back_three, LANES),
        ),
    )
    summed_mlp = lax.psum_scatter(
        mlp_units, "dp", scatter_dimension=0, tiled=True
    ).astype(jnp.float32)
    back_two = gather_rows(back_hidden_two.astype(jnp.bfloat16))
    back_attended = (
        product_right(back_two, mix_w[5]).astype(jnp.bfloat16).reshape(length, local_heads, HEAD)
    )
    lin_again, denom_again, lin_back, win_back = attend(
        query_f, key_f, query_s, key_s, lin_mask, win_mask
    )
    back_prob = jnp.einsum(
        "shd,thd->hst", back_attended, values_v, preferred_element_type=jnp.float32
    )
    back_values = jnp.einsum(
        "hst,shd->thd",
        lin_back.astype(jnp.bfloat16),
        back_attended,
        preferred_element_type=jnp.float32,
    ) + jnp.einsum(
        "hst,shd->thd",
        win_back.astype(jnp.bfloat16),
        back_attended,
        preferred_element_type=jnp.float32,
    )
    back_kernel = (back_prob - jnp.sum(back_prob * lin_back, axis=-1, keepdims=True)) / denom_again
    back_score = (back_kernel * (1.0 + lin_again) * lin_mask).astype(jnp.bfloat16)
    back_query_f = jnp.einsum(
        "hst,thf->shf", back_score, key_f, preferred_element_type=jnp.float32
    ) / math.sqrt(FEAT)
    back_key_f = jnp.einsum(
        "hst,shf->thf", back_score, query_f, preferred_element_type=jnp.float32
    ) / math.sqrt(FEAT)
    back_local = (
        win_back * (back_prob - jnp.sum(back_prob * win_back, axis=-1, keepdims=True))
    ).astype(jnp.bfloat16)
    back_query_s = jnp.einsum(
        "hst,thd->shd", back_local, key_s, preferred_element_type=jnp.float32
    ) / math.sqrt(HEAD)
    back_key_s = jnp.einsum(
        "hst,shd->thd", back_local, query_s, preferred_element_type=jnp.float32
    ) / math.sqrt(HEAD)
    back_projected = [
        piece_grad.reshape(length, -1).astype(jnp.bfloat16)
        for piece_grad in (back_query_f, back_key_f, back_query_s, back_key_s, back_values)
    ]
    back_normed_two = product_right(back_projected[0], mix_w[0])
    for piece_grad, weight in zip(back_projected[1:], mix_w[1:5]):
        back_normed_two = back_normed_two + product_right(piece_grad, weight)
    back_normed_two = sum_rows(back_normed_two)
    back_norm_two, gain_two = norm_back(hidden_one, params[1], back_normed_two)
    back_hidden_one = back_hidden_two + back_norm_two
    mix_units = grad_units(
        owners * cap_mix,
        slot_mix,
        (
            (mix_in, back_projected[0], 7 * LANES),
            (mix_in, back_projected[1], 7 * LANES),
            *[(mix_in, piece_grad, 2 * LANES) for piece_grad in back_projected[2:]],
            (mix_out, back_two, LANES),
        ),
    )
    back_one = gather_rows(back_hidden_one.astype(jnp.bfloat16))
    back_gated = product_right(back_one, conv_w[2])
    back_mixed = back_gated * gate_c
    back_gate_c = (back_gated * mixed_c).astype(jnp.bfloat16)
    back_value_f = taps_local[0] * back_mixed
    tap_grads = [jnp.sum(back_mixed * value_c, axis=0)]
    for shift_by in range(1, TAPS):
        masked = back_mixed * same_prev[shift_by]
        back_value_f = back_value_f + taps_local[shift_by] * advanced(masked, shift_by)
        tap_grads.append(jnp.sum(masked * delayed(value_c, shift_by), axis=0))
    back_value_c = back_value_f.astype(jnp.bfloat16)
    back_normed_one = sum_rows(
        product_right(back_value_c, conv_w[0]) + product_right(back_gate_c, conv_w[1])
    )
    back_norm_one, gain_one = norm_back(x_rows, params[0], back_normed_one)
    grad_input = back_hidden_one + back_norm_one
    conv_units = grad_units(
        owners * cap_conv,
        slot_conv,
        (
            (conv_in, back_value_c, 2 * LANES),
            (conv_in, back_gate_c, 2 * LANES),
            (gated_conv, back_one, LANES),
        ),
    )
    taps_full = lax.dynamic_update_slice(
        jnp.zeros((TAPS, D), jnp.float32), jnp.stack(tap_grads), (jnp.int32(0), column)
    )
    small_grad = jnp.concatenate([jnp.stack([gain_one, gain_two, gain_three]), taps_full], axis=0)
    summed_mix, summed_conv, small_summed = scatter_sum(
        (mix_units, conv_units), small_grad, owners, (cap_mix, cap_conv)
    )
    new_conv = adam_units(state_conv, summed_conv, slot_conv, CONV_SCALE / owners)
    new_mix = adam_units(state_mix, summed_mix, slot_mix, MIX_SCALE / owners)
    new_mlp = adam_units(state_mlp, summed_mlp, slot_mlp, MLP_SCALE / owners)
    small_new = adam_step(small_state, small_summed * (SMALL_SCALE / owners), SMALL_RATE)
    return (
        result,
        grad_input,
        new_conv,
        new_mix,
        new_mlp,
        small_new[1:],
        small_new[0] - small_state[0],
    )


def solution(mesh):
    placed = (
        P(("dp", "tensor"), None),
        P(("dp", "tensor"), None),
        P("dp", None),
        P(),
        P(),
        P(),
        P(None, "dp", "tensor"),
        P(None, "dp", "tensor"),
        P(None, "dp", "tensor"),
        P(),
    )
    return jax.shard_map(
        per_device,
        mesh=mesh,
        in_specs=placed,
        out_specs=(
            P(("dp", "tensor"), None),
            P(("dp", "tensor"), None),
            P(None, "dp", "tensor"),
            P(None, "dp", "tensor"),
            P(None, "dp", "tensor"),
            P(),
            P(),
        ),
        check_vma=False,
    )
```

```python
import math

import functools

import jax
import jax.numpy as jnp
from jax import lax
from jax.experimental import pallas as pl
from jax.experimental.pallas import tpu as pltpu
from jax.sharding import PartitionSpec as P

MESH = pl.DeviceIdType.MESH
LANES = 128

D = 1792
HEADS = 16
FEAT = 16
FF = 4864
WINDOW = 64
TAPS = 3
STEP = 5
HEAD = 112


NORM_EPS = 1e-05
BETA_ONE = 0.9
BETA_TWO = 0.95
ADAM_EPS = 1e-08
LEARN_RATE = 0.02
SMALL_RATE = 0.16
WEIGHT_DECAY = 0.1
NEG_FILL = -1e30
CONV_SCALE = 0.125
MIX_SCALE = 0.25
MLP_SCALE = 0.5
SMALL_SCALE = 0.125


def norm_rows(values, gain):
    return values * lax.rsqrt(jnp.mean(values * values, axis=-1, keepdims=True) + NORM_EPS) * gain


def norm_back(values, gain, upstream):
    _, pullback = jax.vjp(norm_rows, values, gain)
    return pullback(upstream)


def product(left, right):
    return jnp.dot(left, right, preferred_element_type=jnp.float32)


def product_left(left, right):
    return lax.dot_general(
        left, right, (((0,), (0,)), ((), ())), preferred_element_type=jnp.float32
    )


def product_right(left, right):
    return lax.dot_general(
        left, right, (((1,), (1,)), ((), ())), preferred_element_type=jnp.float32
    )


def swap(values, axis, bit):
    size = lax.axis_size(axis)
    return lax.ppermute(values, axis, [(i, i ^ bit) for i in range(size)])


def gather_rows(piece_rows):
    other = swap(piece_rows, "tensor", 1)
    first = lax.axis_index("tensor") == 0
    return jnp.concatenate(
        [jnp.where(first, piece_rows, other), jnp.where(first, other, piece_rows)]
    )


def sum_rows(piece_rows):
    rows = piece_rows.shape[0] // 2
    at = lax.axis_index("tensor")
    halves = piece_rows.astype(jnp.bfloat16).reshape(2, rows, piece_rows.shape[1])
    other = swap(lax.dynamic_index_in_dim(halves, 1 - at, 0, False), "tensor", 1)
    mine = lax.dynamic_index_in_dim(halves, at, 0, False)
    return mine.astype(jnp.float32) + other.astype(jnp.float32)


def delayed(values, steps):
    return jnp.pad(values, ((steps, 0), (0, 0)))[: values.shape[0]]


def advanced(values, steps):
    return jnp.pad(values, ((0, steps), (0, 0)))[steps:]


def lay_body(parts, slots_ref, pooled_ref, *refs):
    out_refs, (buf, stage, sem) = refs[: len(parts)], refs[len(parts) :]
    step = pl.program_id(0)
    depth = buf.shape[2]
    starts = [sum(part[4] for part in parts[:p]) for p in range(len(parts))]

    def inside(at, p):
        return (at >= starts[p]) & (at < starts[p] + parts[p][4])

    def fetch(at, half):
        for p, (first, nu, blocks, _, _) in enumerate(parts):

            @pl.when(inside(at, p))
            def _():
                for q in range(nu * blocks):
                    unit = first + (at - starts[p]) * (nu * blocks) + q
                    pltpu.make_async_copy(
                        pooled_ref.at[slots_ref[unit]], buf.at[half, q], sem.at[half]
                    ).start()

    @pl.when(step == 0)
    def _():
        fetch(0, 0)

    @pl.when(step + 1 < pl.num_programs(0))
    def _():
        fetch(step + 1, (step + 1) % 2)

    half = step % 2
    for p, (first, nu, blocks, m, _) in enumerate(parts):
        out_ref = out_refs[p]
        rows = nu * depth // m

        @pl.when(inside(step, p))
        def _():
            pltpu.make_async_copy(
                pooled_ref.at[pl.ds(0, nu * blocks)], buf.at[half, pl.ds(0, nu * blocks)], sem.at[half]
            ).wait()
            for block in range(blocks):
                if m == 1:
                    for q in range(nu):
                        at = (block * nu + q) * depth
                        out_ref[at : at + depth, :] = buf[half, block * nu + q]
                    continue
                base = (block % 2) * stage.shape[0] // 2
                for q in range(nu):
                    at = base + q * depth
                    stage[at : at + depth, :] = buf[half, block * nu + q].astype(jnp.float32)
                for c in range(m):
                    out_ref[block * rows : (block + 1) * rows, c * LANES : (c + 1) * LANES] = stage[
                        pl.ds(base + c, rows, stride=m), :
                    ].astype(jnp.bfloat16)


def lay_out(pooled, slots, wanted):
    depth = pooled.shape[1]
    parts, specs, shapes = [], [], []
    first = start = 0
    for count, width, nu, blocks in wanted:
        m = width // LANES
        steps = count // (nu * blocks)
        rows = nu * blocks * depth // m
        assert steps * nu * blocks == count
        parts.append((first, nu, blocks, m, steps))

        def place(i, s, start=start, steps=steps):
            return (jnp.clip(i - start, 0, steps - 1), 0)

        specs.append(pl.BlockSpec((rows, width), place))
        shapes.append(jax.ShapeDtypeStruct((steps * rows, width), jnp.bfloat16))
        first += count
        start += steps
    return pl.pallas_call(
        functools.partial(lay_body, tuple(parts)),
        grid_spec=pltpu.PrefetchScalarGridSpec(
            num_scalar_prefetch=1,
            grid=(start,),
            in_specs=[pl.BlockSpec(memory_space=pl.ANY)],
            out_specs=specs,
            scratch_shapes=[
                pltpu.VMEM((2, max(p[1] * p[2] for p in parts), depth, LANES), jnp.bfloat16),
                pltpu.VMEM((2 * max(p[1] for p in parts) * depth, LANES), jnp.float32),
                pltpu.SemaphoreType.DMA((2,)),
            ],
        ),
        out_shape=shapes,
        cost_estimate=pl.CostEstimate(
            flops=0, bytes_accessed=4 * first * depth * LANES, transcendentals=0
        ),
        name=f"lay_{first}",
    )(slots, pooled)


def grad_body(parts, sources, slots_ref, *refs):
    ins, out_ref, stage = refs[:sources], refs[sources], refs[sources + 1]
    bufs, sem = refs[sources + 2 : -1], refs[-1]
    depth = LANES

    def drain(p, half):
        nu = bufs[p].shape[1]
        pltpu.make_async_copy(out_ref.at[pl.ds(0, nu)], bufs[p].at[half], sem.at[p, half]).wait()

    for p, (first, rows, left, right) in enumerate(parts):
        u_ref, d_ref, buf = ins[left], ins[right], bufs[p]
        m = d_ref.shape[1] // LANES
        nu = rows * m // depth

        def step_of(step, carry):
            half = step % 2

            @pl.when(step >= 2)
            def _():
                drain(p, half)

            at = pl.multiple_of(step * rows, LANES)
            turned = u_ref[:, pl.ds(at, rows)].T
            for c in range(0, m, 2):
                wide = min(2, m - c)
                piece = jnp.dot(
                    turned,
                    d_ref[:, c * LANES : (c + wide) * LANES],
                    preferred_element_type=jnp.float32,
                )
                for k in range(wide):
                    part = piece[:, k * LANES : (k + 1) * LANES]
                    if m == 1:
                        stage[:rows, :] = part
                    else:
                        stage[pl.ds(c + k, rows, stride=m), :] = part
            for q in range(nu):
                buf[half, q] = stage[q * depth : (q + 1) * depth, :].astype(jnp.bfloat16)
            for q in range(nu):
                pltpu.make_async_copy(
                    buf.at[half, q], out_ref.at[slots_ref[first + step * nu + q]], sem.at[p, half]
                ).start()
            return carry

        lax.fori_loop(0, u_ref.shape[1] // rows, step_of, 0)
    for p, (first, rows, left, right) in enumerate(parts):
        steps = ins[left].shape[1] // rows
        drain(p, (steps - 1) % 2)
        if steps > 1:
            drain(p, steps % 2)


def grad_units(slot_rows, slots, wanted):
    operands, parts, bufs = [], [], []
    first = most = flops = 0
    where = {}
    for u, d, rows in wanted:
        for value in (u, d):
            if id(value) not in where:
                where[id(value)] = len(operands)
                operands.append(value)
        height, width = u.shape[1], d.shape[1]
        nu = rows * width // LANES // LANES
        parts.append((first, rows, where[id(u)], where[id(d)]))
        bufs.append(pltpu.VMEM((2, nu, LANES, LANES), jnp.bfloat16))
        first += height * width // LANES // LANES
        most = max(most, nu)
        flops += 2 * u.shape[0] * height * width
    return pl.pallas_call(
        functools.partial(grad_body, tuple(parts), len(operands)),
        grid_spec=pltpu.PrefetchScalarGridSpec(
            num_scalar_prefetch=1,
            in_specs=[pl.BlockSpec(memory_space=pltpu.VMEM)] * len(operands),
            out_specs=pl.BlockSpec(memory_space=pl.ANY),
            scratch_shapes=[
                pltpu.VMEM((most * LANES, LANES), jnp.float32),
                *bufs,
                pltpu.SemaphoreType.DMA((len(parts), 2)),
            ],
        ),
        out_shape=jax.ShapeDtypeStruct((slot_rows, LANES, LANES), jnp.bfloat16),
        cost_estimate=pl.CostEstimate(
            flops=flops, bytes_accessed=2 * first * LANES * LANES, transcendentals=0
        ),
        name=f"grad_{first}",
    )(slots, *operands)


def bits_of(owners):
    return owners.bit_length() - 1


def chunks_of(total, most):
    number = -(-total // most)
    base, extra = divmod(total, number)
    out, at = [], 0
    for k in range(number):
        size = base + (1 if k < extra else 0)
        out.append((at, size))
        at += size
    return out


def scatter_body(owners, caps, jobs, *refs):
    stages = bits_of(owners)
    groups = len(caps)
    g_refs, small_ref = refs[:groups], refs[groups]
    out_refs, small_out = refs[groups + 1 : 2 * groups + 1], refs[2 * groups + 1]
    refs = refs[2 * groups + 2 :]
    landing = [refs[s * groups : (s + 1) * groups] for s in range(stages)]
    own, small_sum, small_land, send_sem, recv_sem, own_sem, small_send, small_recv = refs[
        stages * groups :
    ]
    me = lax.axis_index("dp")
    ten = lax.axis_index("tensor")
    bit = [(me // (1 << s)) % 2 for s in range(stages)]
    partner = [me + (1 - 2 * bit[s]) * (1 << s) for s in range(stages)]
    barrier = pltpu.get_barrier_semaphore()
    for s in range(stages):
        pl.semaphore_signal(barrier, inc=1, device_id=(partner[s], ten), device_id_type=MESH)
    pl.semaphore_signal(barrier, inc=1, device_id=(me, 1 - ten), device_id_type=MESH)
    pl.semaphore_wait(barrier, stages + 1)
    count = len(jobs)

    def small(s):
        to = (me, 1 - ten) if s == stages else (partner[s], ten)
        return pltpu.make_async_remote_copy(
            src_ref=small_ref if s == 0 else small_sum.at[s - 1],
            dst_ref=small_land.at[s],
            send_sem=small_send.at[s],
            recv_sem=small_recv.at[s],
            device_id=to,
            device_id_type=MESH,
        )

    def small_step(s):
        small(s).wait_recv()
        total = (small_ref[...] if s == 0 else small_sum[s - 1]) + small_land[s]
        if s == stages:
            small_out[...] = total
        else:
            small_sum[s] = total
            small(s + 1).start()

    small(0).start()

    def bit_at(s, k):
        if jobs[k][3] and s in (1, 2):
            return 3 - s
        return s

    def sides(s, k):
        before = owners >> s
        inner = 2 if jobs[k][3] and s == 1 else 1
        return before // 2 // inner, inner

    def part(s, k, which):
        g, at, size, _ = jobs[k]
        outer, inner = sides(s, k)
        span = pl.ds(at, size)
        if s == 0:
            return g_refs[g].at[:, which, span]
        ref = landing[s - 1][g]
        view = ref.reshape(outer, 2, inner, *ref.shape[1:])
        return view.at[:, which, :, span]

    def remote(s, k):
        g, at, size, _ = jobs[k]
        outer, inner = sides(s, k)
        span = pl.ds(at, size)
        b = bit_at(s, k)
        ref = landing[s][g]
        dst = ref.at[:, span] if s == 0 else ref.reshape(outer, inner, *ref.shape[1:]).at[:, :, span]
        return pltpu.make_async_remote_copy(
            src_ref=part(s, k, 1 - bit[b]),
            dst_ref=dst,
            send_sem=send_sem.at[s, k],
            recv_sem=recv_sem.at[s, k],
            device_id=(partner[b], ten),
            device_id_type=MESH,
        )

    def local(k):
        return pltpu.make_async_copy(
            part(0, k, bit[0]), own.at[k % 2, :, pl.ds(0, jobs[k][2])], own_sem.at[k % 2]
        )

    for k in range(count):
        remote(0, k).start()
    local(0).start()

    def work(s, k):
        g, at, size, _ = jobs[k]
        left = owners >> (s + 1)
        outer, inner = sides(s, k)
        if s == 0:
            if k + 1 < count:
                local(k + 1).start()
            local(k).wait()
        remote(s, k).wait_recv()
        mine_bit = bit[bit_at(s, k)]
        into = landing[s][g]

        def add(j, carry):
            o, u = j // size, j % size
            if s == 0:
                mine = own[k % 2, o, u]
            else:
                mine = landing[s - 1][g][(o // inner) * 2 * inner + mine_bit * inner + o % inner, at + u]
            total = into[o, at + u].astype(jnp.float32) + mine.astype(jnp.float32)
            if s == stages - 1:
                out_refs[g][at + u] = total
            else:
                into[o, at + u] = total.astype(jnp.bfloat16)
            return carry

        lax.fori_loop(0, left * size, add, 0)
        if s + 1 < stages:
            remote(s + 1, k).start()

    lag = 2
    for t in range(count + lag * (stages - 1)):
        for s in range(stages):
            k = t - lag * s
            if 0 <= k < count:
                work(s, k)
        if t % 2 == 1 and t // 2 <= stages:
            small_step(t // 2)
    for s in range(stages):
        for k in range(count):
            remote(s, k).wait_send()
    for s in range(stages + 1):
        small(s).wait_send()


def scatter_sum(units, small, owners, caps, collective=1, most=4):
    stages = bits_of(owners)
    depth, lanes = units[0].shape[1:]
    jobs = []
    for g, cap in enumerate(caps):
        for at, size in chunks_of(cap, most):
            jobs.append((g, at, size, stages > 2 and len(jobs) % 4 == 2))
    widest = max(size for _, _, size, _ in jobs)
    assert len(jobs) + 2 * (stages - 1) > 2 * stages + 1
    scratch = []
    for s in range(stages):
        for cap in caps:
            scratch.append(pltpu.VMEM((owners >> (s + 1), cap, depth, lanes), jnp.bfloat16))
    scratch += [
        pltpu.VMEM((2, owners // 2, widest, depth, lanes), jnp.bfloat16),
        pltpu.VMEM((stages, *small.shape), jnp.float32),
        pltpu.VMEM((stages + 1, *small.shape), jnp.float32),
        pltpu.SemaphoreType.DMA((stages, len(jobs))),
        pltpu.SemaphoreType.DMA((stages, len(jobs))),
        pltpu.SemaphoreType.DMA((2,)),
        pltpu.SemaphoreType.DMA((stages + 1,)),
        pltpu.SemaphoreType.DMA((stages + 1,)),
    ]
    return pl.pallas_call(
        functools.partial(scatter_body, owners, caps, tuple(jobs)),
        out_shape=[
            *[jax.ShapeDtypeStruct((cap, depth, lanes), jnp.float32) for cap in caps],
            jax.ShapeDtypeStruct(small.shape, jnp.float32),
        ],
        in_specs=[
            *[pl.BlockSpec(memory_space=pl.ANY)] * len(caps),
            pl.BlockSpec(memory_space=pltpu.VMEM),
        ],
        out_specs=[pl.BlockSpec(memory_space=pltpu.VMEM)] * (len(caps) + 1),
        scratch_shapes=scratch,
        compiler_params=pltpu.CompilerParams(collective_id=collective, has_side_effects=True),
        name="scatter_sum",
    )(
        *[group.reshape(owners // 2, 2, cap, depth, lanes) for group, cap in zip(units, caps)],
        small,
    )


def adam_values(master, one, two, gradient, rate):
    moment_one = BETA_ONE * one + (1.0 - BETA_ONE) * gradient
    moment_two = BETA_TWO * two + (1.0 - BETA_TWO) * gradient * gradient
    step_size = (
        moment_one
        / (1.0 - BETA_ONE**STEP)
        / (jnp.sqrt(moment_two / (1.0 - BETA_TWO**STEP)) + ADAM_EPS)
    )
    return master - rate * (step_size + WEIGHT_DECAY * master), moment_one, moment_two


def adam_step(opt_state, gradient, rate):
    return jnp.stack(adam_values(opt_state[0], opt_state[1], opt_state[2], gradient, rate))


def adam_body(scale, used_ref, state_ref, summed_ref, out_ref, *scratch):
    cap, rows, lanes = summed_ref.shape
    if scratch:
        scratch[0][...] = summed_ref[...].astype(jnp.float32)
        summed_ref = scratch[0]
    flat = summed_ref.reshape(cap * rows, lanes)
    used = used_ref[...] > 0
    for r in range(rows):
        here = slice(r * lanes, (r + 1) * lanes)
        summed = flat[pl.ds(r, cap, stride=rows), :] * scale
        gradient = jnp.where(used, summed, 0.0)
        new = adam_values(
            state_ref[0, :, here], state_ref[1, :, here], state_ref[2, :, here], gradient, LEARN_RATE
        )
        for k in range(3):
            out_ref[k, :, here] = new[k]


def adam_units(state, summed, slots, scale):
    cap, unit_width = state.shape[1:]
    mine = lax.axis_index("dp") * cap + jnp.arange(cap, dtype=jnp.int32)
    used = jnp.any(mine[:, None] == slots[None, :], axis=1).astype(jnp.int32)
    rows = 16
    block = rows * LANES
    return pl.pallas_call(
        functools.partial(adam_body, scale),
        grid=(unit_width // block,),
        in_specs=[
            pl.BlockSpec((cap, LANES), lambda i: (0, 0)),
            pl.BlockSpec((3, cap, block), lambda i: (0, 0, i)),
            pl.BlockSpec((cap, rows, LANES), lambda i: (0, i, 0)),
        ],
        out_specs=pl.BlockSpec((3, cap, block), lambda i: (0, 0, i)),
        out_shape=jax.ShapeDtypeStruct(state.shape, jnp.float32),
        scratch_shapes=[pltpu.VMEM((cap, rows, LANES), jnp.float32)]
        if summed.dtype == jnp.bfloat16
        else [],
        name=f"adam_{cap}",
    )(jnp.broadcast_to(used[:, None], (cap, LANES)), state, summed)


def spread_body(owners, cap, jobs, own_ref, out_ref, local_sem, send_sem, recv_sem):
    stages = bits_of(owners)
    me = lax.axis_index("dp")
    ten = lax.axis_index("tensor")
    bit = [(me // (1 << s)) % 2 for s in range(stages)]
    partner = [me + (1 - 2 * bit[s]) * (1 << s) for s in range(stages)]
    barrier = pltpu.get_barrier_semaphore()
    for s in range(stages):
        pl.semaphore_signal(barrier, inc=1, device_id=(partner[s], ten), device_id_type=MESH)
    pl.semaphore_wait(barrier, stages)
    tail = out_ref.shape[2:]

    def bit_at(s, k):
        b = stages - 1 - s
        return 3 - b if jobs[k][2] and b in (1, 2) else b

    def held(s, k):
        at, size, swapped = jobs[k]
        span = pl.ds(at, size)
        b = stages - 1 - s
        if swapped and b == 2:
            return out_ref.reshape(owners >> 3, 8, cap, *tail).at[:, me % 8, span]
        if swapped and b == 1:
            view = out_ref.reshape(owners >> 3, 2, 2, 2, cap, *tail)
            return view.at[:, bit[2], :, bit[0], span]
        low = 1 << (b + 1)
        return out_ref.reshape(owners // low, low, cap, *tail).at[:, me % low, span]

    def remote(s, k):
        b = bit_at(s, k)
        at, size, _ = jobs[k]
        dst = out_ref.at[me, pl.ds(at, size)] if s == 0 else held(s, k)
        return pltpu.make_async_remote_copy(
            src_ref=own_ref.at[pl.ds(at, size)] if s == 0 else dst,
            dst_ref=dst,
            send_sem=send_sem.at[s, k],
            recv_sem=recv_sem.at[s, k],
            device_id=(partner[b], ten),
            device_id_type=MESH,
        )

    local = pltpu.make_async_copy(own_ref, out_ref.at[me], local_sem.at[0])
    count = len(jobs)
    for k in range(count):
        remote(0, k).start()
    local.start()
    local.wait()
    for t in range(count + stages - 1):
        for s in range(stages):
            k = t - s
            if 0 <= k < count:
                remote(s, k).wait_recv()
                if s + 1 < stages:
                    remote(s + 1, k).start()
    for s in range(stages):
        for k in range(count):
            remote(s, k).wait_send()


def spread_units(own, owners, collective, most=4):
    cap, depth, lanes = own.shape
    stages = bits_of(owners)
    jobs = tuple(
        (at, size, stages > 2 and number % 4 == 2)
        for number, (at, size) in enumerate(chunks_of(cap, most))
    )
    out = pl.pallas_call(
        functools.partial(spread_body, owners, cap, jobs),
        out_shape=jax.ShapeDtypeStruct((owners, cap, depth, lanes), jnp.bfloat16),
        in_specs=[pl.BlockSpec(memory_space=pltpu.VMEM)],
        out_specs=pl.BlockSpec(memory_space=pl.ANY),
        scratch_shapes=[
            pltpu.SemaphoreType.DMA((1,)),
            pltpu.SemaphoreType.DMA((stages, len(jobs))),
            pltpu.SemaphoreType.DMA((stages, len(jobs))),
        ],
        compiler_params=pltpu.CompilerParams(collective_id=collective, has_side_effects=True),
        name=f"spread_{cap}",
    )(own)
    return out.reshape(owners * cap, depth, lanes)


def own_units(state, scale):
    cap, unit_width = state.shape[1:]
    return (state[0] * scale).reshape(cap, unit_width // LANES, LANES).astype(jnp.bfloat16)


def attend(query_f, key_f, query_s, key_s, lin_mask, win_mask):
    lin_score = jnp.einsum(
        "shf,thf->hst", query_f, key_f, preferred_element_type=jnp.float32
    ) / math.sqrt(FEAT)
    kernel = (1.0 + lin_score + 0.5 * lin_score * lin_score) * lin_mask
    lin_denom = jnp.sum(kernel, axis=-1, keepdims=True)
    lin_prob = kernel / lin_denom
    win_score = jnp.einsum(
        "shd,thd->hst", query_s, key_s, preferred_element_type=jnp.float32
    ) / math.sqrt(HEAD)
    inside = win_mask > 0
    win_peak = jnp.max(jnp.where(inside, win_score, NEG_FILL), axis=-1, keepdims=True)
    win_exp = jnp.exp(jnp.where(inside, win_score - win_peak, NEG_FILL))
    win_prob = win_exp / jnp.sum(win_exp, axis=-1, keepdims=True)
    return (lin_score, lin_denom, lin_prob, win_prob)


def per_device(
    inputs,
    cotangent,
    segments,
    slot_conv,
    slot_mix,
    slot_mlp,
    state_conv,
    state_mix,
    state_mlp,
    small_state,
):
    tensor_size = lax.axis_size("tensor")
    owners = lax.axis_size("dp")
    half_width = D // tensor_size
    local_heads = HEADS // tensor_size
    feat_cols = local_heads * FEAT
    ff_half = FF // tensor_size
    unit_width = state_conv.shape[2]
    cap_conv = state_conv.shape[1]
    cap_mix = state_mix.shape[1]
    cap_mlp = state_mlp.shape[1]
    own_conv, own_mix, own_mlp = lax.optimization_barrier(
        (
            own_units(state_conv, CONV_SCALE),
            own_units(state_mix, MIX_SCALE),
            own_units(state_mlp, MLP_SCALE),
        )
    )
    pooled = (
        spread_units(own_conv, owners, 2),
        lax.all_gather(own_mix, "dp", axis=0, tiled=True),
        lax.all_gather(own_mlp, "dp", axis=0, tiled=True),
    )
    per = D * LANES // unit_width
    narrow, middle = per * feat_cols // LANES, per * half_width // LANES
    wide = per * ff_half // LANES
    conv_pair, conv_back = lay_out(
        pooled[0], slot_conv, ((2 * middle, half_width, 7, 2), (middle, D, 7, 2))
    )
    conv_w = [conv_pair[:D], conv_pair[D:], conv_back]
    feat_pair, mix_trio, mix_back = lay_out(
        pooled[1],
        slot_mix,
        ((2 * narrow, feat_cols, 7, 2), (3 * middle, half_width, 7, 3), (middle, D, 7, 2)),
    )
    mix_w = [
        feat_pair[:D],
        feat_pair[D:],
        mix_trio[:D],
        mix_trio[D : 2 * D],
        mix_trio[2 * D :],
        mix_back,
    ]
    mlp_pair, mlp_back = lay_out(
        pooled[2], slot_mlp, ((2 * wide, ff_half, 19, 2), (wide, D, 7, 2))
    )
    mlp_w = [mlp_pair[:D], mlp_pair[D:], mlp_back]
    params = small_state[0] * SMALL_SCALE
    seg_ids = segments[0]
    length = seg_ids.shape[0]
    positions = jnp.arange(length)
    causal = (positions[:, None] >= positions[None, :]) & (seg_ids[:, None] == seg_ids[None, :])
    lin_mask = causal.astype(jnp.float32)
    win_mask = (causal & (positions[:, None] - positions[None, :] < WINDOW)).astype(jnp.float32)
    same_prev = [None]
    for shift_by in range(1, TAPS):
        earlier = jnp.pad(seg_ids, (shift_by, 0), constant_values=-1)[:length]
        same_prev.append((earlier == seg_ids).astype(jnp.float32)[:, None])
    column = lax.axis_index("tensor") * half_width
    taps_local = lax.dynamic_slice_in_dim(params[3:], column, half_width, 1)
    x_rows = inputs.astype(jnp.float32)
    normed_one = norm_rows(x_rows, params[0]).astype(jnp.bfloat16)
    conv_in = gather_rows(normed_one)
    value_c = product(conv_in, conv_w[0])
    gate_c = product(conv_in, conv_w[1])
    mixed_c = taps_local[0] * value_c
    for shift_by in range(1, TAPS):
        mixed_c = mixed_c + taps_local[shift_by] * delayed(value_c, shift_by) * same_prev[shift_by]
    gated_conv = (mixed_c * gate_c).astype(jnp.bfloat16)
    hidden_one = x_rows + sum_rows(product(gated_conv, conv_w[2]))
    normed_two = norm_rows(hidden_one, params[1]).astype(jnp.bfloat16)
    mix_in = gather_rows(normed_two)
    projected = [product(mix_in, weight).astype(jnp.bfloat16) for weight in mix_w[:5]]
    query_f = projected[0].reshape(length, local_heads, FEAT)
    key_f = projected[1].reshape(length, local_heads, FEAT)
    query_s = projected[2].reshape(length, local_heads, HEAD)
    key_s = projected[3].reshape(length, local_heads, HEAD)
    values_v = projected[4].reshape(length, local_heads, HEAD)
    _, _, lin_prob, win_prob = attend(query_f, key_f, query_s, key_s, lin_mask, win_mask)
    attended = jnp.einsum(
        "hst,thd->shd", lin_prob.astype(jnp.bfloat16), values_v, preferred_element_type=jnp.float32
    ) + jnp.einsum(
        "hst,thd->shd", win_prob.astype(jnp.bfloat16), values_v, preferred_element_type=jnp.float32
    )
    mix_out = attended.reshape(length, half_width).astype(jnp.bfloat16)
    hidden_two = hidden_one + sum_rows(product(mix_out, mix_w[5]))
    normed_three = norm_rows(hidden_two, params[2]).astype(jnp.bfloat16)
    ff_in = gather_rows(normed_three)
    gate_proj = product(ff_in, mlp_w[0])
    up_proj = product(ff_in, mlp_w[1])
    activated = (jax.nn.silu(gate_proj) * up_proj).astype(jnp.bfloat16)
    result = (hidden_two + sum_rows(product(activated, mlp_w[2]))).astype(jnp.bfloat16)
    back_three = gather_rows(cotangent)
    back_act = product_right(back_three, mlp_w[2])
    gate_sig = jax.nn.sigmoid(gate_proj)
    back_gate = (back_act * up_proj * gate_sig * (1.0 + gate_proj * (1.0 - gate_sig))).astype(
        jnp.bfloat16
    )
    back_up = (back_act * gate_proj * gate_sig).astype(jnp.bfloat16)
    back_normed_three = sum_rows(
        product_right(back_gate, mlp_w[0]) + product_right(back_up, mlp_w[1])
    )
    back_norm_three, gain_three = norm_back(hidden_two, params[2], back_normed_three)
    back_hidden_two = cotangent.astype(jnp.float32) + back_norm_three
    mlp_units = grad_units(
        owners * cap_mlp,
        slot_mlp,
        (
            (ff_in, back_gate, 2 * LANES),
            (ff_in, back_up, 2 * LANES),
            (activated, back_three, LANES),
        ),
    )
    summed_mlp = lax.psum_scatter(mlp_units, "dp", scatter_dimension=0, tiled=True)
    back_two = gather_rows(back_hidden_two.astype(jnp.bfloat16))
    back_attended = (
        product_right(back_two, mix_w[5]).astype(jnp.bfloat16).reshape(length, local_heads, HEAD)
    )
    lin_again, denom_again, lin_back, win_back = attend(
        query_f, key_f, query_s, key_s, lin_mask, win_mask
    )
    back_prob = jnp.einsum(
        "shd,thd->hst", back_attended, values_v, preferred_element_type=jnp.float32
    )
    back_values = jnp.einsum(
        "hst,shd->thd",
        lin_back.astype(jnp.bfloat16),
        back_attended,
        preferred_element_type=jnp.float32,
    ) + jnp.einsum(
        "hst,shd->thd",
        win_back.astype(jnp.bfloat16),
        back_attended,
        preferred_element_type=jnp.float32,
    )
    back_kernel = (back_prob - jnp.sum(back_prob * lin_back, axis=-1, keepdims=True)) / denom_again
    back_score = (back_kernel * (1.0 + lin_again) * lin_mask).astype(jnp.bfloat16)
    back_query_f = jnp.einsum(
        "hst,thf->shf", back_score, key_f, preferred_element_type=jnp.float32
    ) / math.sqrt(FEAT)
    back_key_f = jnp.einsum(
        "hst,shf->thf", back_score, query_f, preferred_element_type=jnp.float32
    ) / math.sqrt(FEAT)
    back_local = (
        win_back * (back_prob - jnp.sum(back_prob * win_back, axis=-1, keepdims=True))
    ).astype(jnp.bfloat16)
    back_query_s = jnp.einsum(
        "hst,thd->shd", back_local, key_s, preferred_element_type=jnp.float32
    ) / math.sqrt(HEAD)
    back_key_s = jnp.einsum(
        "hst,shd->thd", back_local, query_s, preferred_element_type=jnp.float32
    ) / math.sqrt(HEAD)
    back_projected = [
        piece_grad.reshape(length, -1).astype(jnp.bfloat16)
        for piece_grad in (back_query_f, back_key_f, back_query_s, back_key_s, back_values)
    ]
    back_normed_two = product_right(back_projected[0], mix_w[0])
    for piece_grad, weight in zip(back_projected[1:], mix_w[1:5]):
        back_normed_two = back_normed_two + product_right(piece_grad, weight)
    back_normed_two = sum_rows(back_normed_two)
    back_norm_two, gain_two = norm_back(hidden_one, params[1], back_normed_two)
    back_hidden_one = back_hidden_two + back_norm_two
    mix_units = grad_units(
        owners * cap_mix,
        slot_mix,
        (
            (mix_in, back_projected[0], 7 * LANES),
            (mix_in, back_projected[1], 7 * LANES),
            *[(mix_in, piece_grad, 2 * LANES) for piece_grad in back_projected[2:]],
            (mix_out, back_two, LANES),
        ),
    )
    back_one = gather_rows(back_hidden_one.astype(jnp.bfloat16))
    back_gated = product_right(back_one, conv_w[2])
    back_mixed = back_gated * gate_c
    back_gate_c = (back_gated * mixed_c).astype(jnp.bfloat16)
    back_value_f = taps_local[0] * back_mixed
    tap_grads = [jnp.sum(back_mixed * value_c, axis=0)]
    for shift_by in range(1, TAPS):
        masked = back_mixed * same_prev[shift_by]
        back_value_f = back_value_f + taps_local[shift_by] * advanced(masked, shift_by)
        tap_grads.append(jnp.sum(masked * delayed(value_c, shift_by), axis=0))
    back_value_c = back_value_f.astype(jnp.bfloat16)
    back_normed_one = sum_rows(
        product_right(back_value_c, conv_w[0]) + product_right(back_gate_c, conv_w[1])
    )
    back_norm_one, gain_one = norm_back(x_rows, params[0], back_normed_one)
    grad_input = back_hidden_one + back_norm_one
    conv_units = grad_units(
        owners * cap_conv,
        slot_conv,
        (
            (conv_in, back_value_c, 2 * LANES),
            (conv_in, back_gate_c, 2 * LANES),
            (gated_conv, back_one, LANES),
        ),
    )
    taps_full = lax.dynamic_update_slice(
        jnp.zeros((TAPS, D), jnp.float32), jnp.stack(tap_grads), (jnp.int32(0), column)
    )
    small_grad = jnp.concatenate([jnp.stack([gain_one, gain_two, gain_three]), taps_full], axis=0)
    summed_mix, summed_conv, small_summed = scatter_sum(
        (mix_units, conv_units), small_grad, owners, (cap_mix, cap_conv)
    )
    new_conv = adam_units(state_conv, summed_conv, slot_conv, CONV_SCALE / owners)
    new_mix = adam_units(state_mix, summed_mix, slot_mix, MIX_SCALE / owners)
    new_mlp = adam_units(state_mlp, summed_mlp, slot_mlp, MLP_SCALE / owners)
    small_new = adam_step(small_state, small_summed * (SMALL_SCALE / owners), SMALL_RATE)
    return (
        result,
        grad_input,
        new_conv,
        new_mix,
        new_mlp,
        small_new[1:],
        small_new[0] - small_state[0],
    )


def solution(mesh):
    placed = (
        P(("dp", "tensor"), None),
        P(("dp", "tensor"), None),
        P("dp", None),
        P(),
        P(),
        P(),
        P(None, "dp", "tensor"),
        P(None, "dp", "tensor"),
        P(None, "dp", "tensor"),
        P(),
    )
    return jax.shard_map(
        per_device,
        mesh=mesh,
        in_specs=placed,
        out_specs=(
            P(("dp", "tensor"), None),
            P(("dp", "tensor"), None),
            P(None, "dp", "tensor"),
            P(None, "dp", "tensor"),
            P(None, "dp", "tensor"),
            P(),
            P(),
        ),
        check_vma=False,
    )
```

```python
import math

import functools

import jax
import jax.numpy as jnp
from jax import lax
from jax.experimental import pallas as pl
from jax.experimental.pallas import tpu as pltpu
from jax.sharding import PartitionSpec as P

MESH = pl.DeviceIdType.MESH
LANES = 128

D = 1792
HEADS = 16
FEAT = 16
FF = 4864
WINDOW = 64
TAPS = 3
STEP = 5
HEAD = 112


NORM_EPS = 1e-05
BETA_ONE = 0.9
BETA_TWO = 0.95
ADAM_EPS = 1e-08
LEARN_RATE = 0.02
SMALL_RATE = 0.16
WEIGHT_DECAY = 0.1
NEG_FILL = -1e30
CONV_SCALE = 0.125
MIX_SCALE = 0.25
MLP_SCALE = 0.5
SMALL_SCALE = 0.125


def norm_rows(values, gain):
    return values * lax.rsqrt(jnp.mean(values * values, axis=-1, keepdims=True) + NORM_EPS) * gain


def norm_back(values, gain, upstream):
    _, pullback = jax.vjp(norm_rows, values, gain)
    return pullback(upstream)


def product(left, right):
    return jnp.dot(left, right, preferred_element_type=jnp.float32)


def product_left(left, right):
    return lax.dot_general(
        left, right, (((0,), (0,)), ((), ())), preferred_element_type=jnp.float32
    )


def product_right(left, right):
    return lax.dot_general(
        left, right, (((1,), (1,)), ((), ())), preferred_element_type=jnp.float32
    )


def swap(values, axis, bit):
    size = lax.axis_size(axis)
    return lax.ppermute(values, axis, [(i, i ^ bit) for i in range(size)])


def gather_rows(piece_rows):
    other = swap(piece_rows, "tensor", 1)
    first = lax.axis_index("tensor") == 0
    return jnp.concatenate(
        [jnp.where(first, piece_rows, other), jnp.where(first, other, piece_rows)]
    )


def sum_rows(piece_rows):
    rows = piece_rows.shape[0] // 2
    at = lax.axis_index("tensor")
    halves = piece_rows.astype(jnp.bfloat16).reshape(2, rows, piece_rows.shape[1])
    other = swap(lax.dynamic_index_in_dim(halves, 1 - at, 0, False), "tensor", 1)
    mine = lax.dynamic_index_in_dim(halves, at, 0, False)
    return mine.astype(jnp.float32) + other.astype(jnp.float32)


def delayed(values, steps):
    return jnp.pad(values, ((steps, 0), (0, 0)))[: values.shape[0]]


def advanced(values, steps):
    return jnp.pad(values, ((0, steps), (0, 0)))[steps:]


def lay_body(parts, slots_ref, pooled_ref, *refs):
    out_refs, (buf, stage, sem) = refs[: len(parts)], refs[len(parts) :]
    step = pl.program_id(0)
    depth = buf.shape[2]
    starts = [sum(part[4] for part in parts[:p]) for p in range(len(parts))]

    def inside(at, p):
        return (at >= starts[p]) & (at < starts[p] + parts[p][4])

    def fetch(at, half):
        for p, (first, nu, blocks, _, _) in enumerate(parts):

            @pl.when(inside(at, p))
            def _():
                for q in range(nu * blocks):
                    unit = first + (at - starts[p]) * (nu * blocks) + q
                    pltpu.make_async_copy(
                        pooled_ref.at[slots_ref[unit]], buf.at[half, q], sem.at[half]
                    ).start()

    @pl.when(step == 0)
    def _():
        fetch(0, 0)

    @pl.when(step + 1 < pl.num_programs(0))
    def _():
        fetch(step + 1, (step + 1) % 2)

    half = step % 2
    for p, (first, nu, blocks, m, _) in enumerate(parts):
        out_ref = out_refs[p]
        rows = nu * depth // m

        @pl.when(inside(step, p))
        def _():
            pltpu.make_async_copy(
                pooled_ref.at[pl.ds(0, nu * blocks)], buf.at[half, pl.ds(0, nu * blocks)], sem.at[half]
            ).wait()
            for block in range(blocks):
                if m == 1:
                    for q in range(nu):
                        at = (block * nu + q) * depth
                        out_ref[at : at + depth, :] = buf[half, block * nu + q]
                    continue
                base = (block % 2) * stage.shape[0] // 2
                for q in range(nu):
                    at = base + q * depth
                    stage[at : at + depth, :] = buf[half, block * nu + q].astype(jnp.float32)
                for c in range(m):
                    out_ref[block * rows : (block + 1) * rows, c * LANES : (c + 1) * LANES] = stage[
                        pl.ds(base + c, rows, stride=m), :
                    ].astype(jnp.bfloat16)


def lay_out(pooled, slots, wanted):
    depth = pooled.shape[1]
    parts, specs, shapes = [], [], []
    first = start = 0
    for count, width, nu, blocks in wanted:
        m = width // LANES
        steps = count // (nu * blocks)
        rows = nu * blocks * depth // m
        assert steps * nu * blocks == count
        parts.append((first, nu, blocks, m, steps))

        def place(i, s, start=start, steps=steps):
            return (jnp.clip(i - start, 0, steps - 1), 0)

        specs.append(pl.BlockSpec((rows, width), place))
        shapes.append(jax.ShapeDtypeStruct((steps * rows, width), jnp.bfloat16))
        first += count
        start += steps
    return pl.pallas_call(
        functools.partial(lay_body, tuple(parts)),
        grid_spec=pltpu.PrefetchScalarGridSpec(
            num_scalar_prefetch=1,
            grid=(start,),
            in_specs=[pl.BlockSpec(memory_space=pl.ANY)],
            out_specs=specs,
            scratch_shapes=[
                pltpu.VMEM((2, max(p[1] * p[2] for p in parts), depth, LANES), jnp.bfloat16),
                pltpu.VMEM((2 * max(p[1] for p in parts) * depth, LANES), jnp.float32),
                pltpu.SemaphoreType.DMA((2,)),
            ],
        ),
        out_shape=shapes,
        cost_estimate=pl.CostEstimate(
            flops=0, bytes_accessed=4 * first * depth * LANES, transcendentals=0
        ),
        name=f"lay_{first}",
    )(slots, pooled)


def ffn_body(wide, slots_ref, pooled_ref, u_ref, y_ref, *refs):
    out_ref, hid_ref, dgt_ref, dup_ref, du_ref = refs[:5]
    first_w, last_w, buf, stage, sem = refs[5:]
    depth = buf.shape[2]
    width, model = u_ref.shape[1], last_w.shape[1]
    hidden = last_w.shape[0]
    ring = buf.shape[0]
    kinds = (
        (0, 2 * wide, hidden // LANES, 1, first_w),
        (2 * wide, wide, model // LANES // 2, 2, last_w),
    )
    steps = [kind[1] // (kind[2] * kind[3]) for kind in kinds]
    total = sum(steps)

    def fetch(at):
        for p, (first, _, nu, blocks, _) in enumerate(kinds):
            begin = sum(steps[:p])

            @pl.when((at >= begin) & (at < begin + steps[p]))
            def _():
                for q in range(nu * blocks):
                    unit = first + (at - begin) * (nu * blocks) + q
                    pltpu.make_async_copy(
                        pooled_ref.at[slots_ref[unit]], buf.at[at % ring, q], sem.at[at % ring]
                    ).start()

    for at in range(ring - 1):
        fetch(jnp.int32(at))
    for p, (first, _, nu, blocks, into) in enumerate(kinds):
        begin = sum(steps[:p])
        m = into.shape[1] // LANES
        rows = nu * depth // m

        def step_of(step, carry):
            at = begin + step
            half = at % ring
            fetch(at + ring - 1)
            pltpu.make_async_copy(
                pooled_ref.at[pl.ds(0, nu * blocks)], buf.at[half, pl.ds(0, nu * blocks)], sem.at[half]
            ).wait()
            for block in range(blocks):
                for q in range(nu):
                    stage[q * depth : (q + 1) * depth, :] = buf[half, block * nu + q].astype(
                        jnp.float32
                    )
                row = pl.multiple_of(step * (rows * blocks) + block * rows, rows)
                for c in range(m):
                    into[pl.ds(row, rows), c * LANES : (c + 1) * LANES] = stage[
                        pl.ds(c, rows, stride=m), :
                    ].astype(jnp.bfloat16)
            return carry

        lax.fori_loop(0, steps[p], step_of, 0)

    def hidden_columns(at, size):
        span = pl.ds(at, size)
        gate = jnp.dot(u_ref[...], first_w[:width, span], preferred_element_type=jnp.float32)
        up = jnp.dot(u_ref[...], first_w[width:, span], preferred_element_type=jnp.float32)
        back = lax.dot_general(
            y_ref[...], last_w[span, :], (((1,), (1,)), ((), ())), preferred_element_type=jnp.float32
        )
        sig = jax.nn.sigmoid(gate)
        hid_ref[:, span] = (gate * sig * up).astype(jnp.bfloat16)
        dgt_ref[:, span] = (back * up * sig * (1.0 + gate * (1.0 - sig))).astype(jnp.bfloat16)
        dup_ref[:, span] = (back * gate * sig).astype(jnp.bfloat16)

    block = 2 * LANES

    def over(extent, run):
        def body(j, carry):
            run(pl.multiple_of(j * block, block), block)
            return carry

        lax.fori_loop(0, extent // block, body, 0)
        if extent % block:
            run(extent - extent % block, extent % block)

    over(hidden, hidden_columns)

    def model_columns(at, size):
        span = pl.ds(at, size)
        back = lax.dot_general(
            dgt_ref[...], first_w[span, :], (((1,), (1,)), ((), ())), preferred_element_type=jnp.float32
        ) + lax.dot_general(
            dup_ref[...],
            first_w[pl.ds(width + at, size), :],
            (((1,), (1,)), ((), ())),
            preferred_element_type=jnp.float32,
        )
        du_ref[:, span] = back.astype(jnp.bfloat16)
        out_ref[:, span] = jnp.dot(
            hid_ref[...], last_w[:, span], preferred_element_type=jnp.float32
        ).astype(jnp.bfloat16)

    over(model, model_columns)


def feed_forward(pooled, slots, wide, u, y, hidden):
    tokens, model = u.shape
    depth = pooled.shape[1]
    small = jax.ShapeDtypeStruct((tokens, model), jnp.bfloat16)
    large = jax.ShapeDtypeStruct((tokens, hidden), jnp.bfloat16)
    nu = max(hidden // LANES, model // LANES)
    return pl.pallas_call(
        functools.partial(ffn_body, wide),
        grid_spec=pltpu.PrefetchScalarGridSpec(
            num_scalar_prefetch=1,
            in_specs=[
                pl.BlockSpec(memory_space=pl.ANY),
                pl.BlockSpec(memory_space=pltpu.VMEM),
                pl.BlockSpec(memory_space=pltpu.VMEM),
            ],
            out_specs=[pl.BlockSpec(memory_space=pltpu.VMEM)] * 5,
            scratch_shapes=[
                pltpu.VMEM((2 * model, hidden), jnp.bfloat16),
                pltpu.VMEM((hidden, model), jnp.bfloat16),
                pltpu.VMEM((4, nu, depth, LANES), jnp.bfloat16),
                pltpu.VMEM((nu * depth, LANES), jnp.float32),
                pltpu.SemaphoreType.DMA((4,)),
            ],
        ),
        out_shape=[small, large, large, large, small],
        cost_estimate=pl.CostEstimate(
            flops=12 * tokens * model * hidden,
            bytes_accessed=6 * model * hidden,
            transcendentals=tokens * hidden,
        ),
        name="feed_forward",
    )(slots, pooled, u, y)


def grad_body(parts, sources, slots_ref, *refs):
    ins, out_ref, stage = refs[:sources], refs[sources], refs[sources + 1]
    bufs, sem = refs[sources + 2 : -1], refs[-1]
    depth = LANES

    def drain(p, half):
        nu = bufs[p].shape[1]
        pltpu.make_async_copy(out_ref.at[pl.ds(0, nu)], bufs[p].at[half], sem.at[p, half]).wait()

    for p, (first, rows, left, right) in enumerate(parts):
        u_ref, d_ref, buf = ins[left], ins[right], bufs[p]
        m = d_ref.shape[1] // LANES
        nu = rows * m // depth

        def step_of(step, carry):
            half = step % 2

            @pl.when(step >= 2)
            def _():
                drain(p, half)

            at = pl.multiple_of(step * rows, LANES)
            turned = u_ref[:, pl.ds(at, rows)].T
            for c in range(0, m, 2):
                wide = min(2, m - c)
                piece = jnp.dot(
                    turned,
                    d_ref[:, c * LANES : (c + wide) * LANES],
                    preferred_element_type=jnp.float32,
                )
                for k in range(wide):
                    part = piece[:, k * LANES : (k + 1) * LANES]
                    if m == 1:
                        stage[:rows, :] = part
                    else:
                        stage[pl.ds(c + k, rows, stride=m), :] = part
            for q in range(nu):
                buf[half, q] = stage[q * depth : (q + 1) * depth, :].astype(jnp.bfloat16)
            for q in range(nu):
                pltpu.make_async_copy(
                    buf.at[half, q], out_ref.at[slots_ref[first + step * nu + q]], sem.at[p, half]
                ).start()
            return carry

        lax.fori_loop(0, u_ref.shape[1] // rows, step_of, 0)
    for p, (first, rows, left, right) in enumerate(parts):
        steps = ins[left].shape[1] // rows
        drain(p, (steps - 1) % 2)
        if steps > 1:
            drain(p, steps % 2)


def grad_units(slot_rows, slots, wanted):
    operands, parts, bufs = [], [], []
    first = most = flops = 0
    where = {}
    for u, d, rows in wanted:
        for value in (u, d):
            if id(value) not in where:
                where[id(value)] = len(operands)
                operands.append(value)
        height, width = u.shape[1], d.shape[1]
        nu = rows * width // LANES // LANES
        parts.append((first, rows, where[id(u)], where[id(d)]))
        bufs.append(pltpu.VMEM((2, nu, LANES, LANES), jnp.bfloat16))
        first += height * width // LANES // LANES
        most = max(most, nu)
        flops += 2 * u.shape[0] * height * width
    return pl.pallas_call(
        functools.partial(grad_body, tuple(parts), len(operands)),
        grid_spec=pltpu.PrefetchScalarGridSpec(
            num_scalar_prefetch=1,
            in_specs=[pl.BlockSpec(memory_space=pltpu.VMEM)] * len(operands),
            out_specs=pl.BlockSpec(memory_space=pl.ANY),
            scratch_shapes=[
                pltpu.VMEM((most * LANES, LANES), jnp.float32),
                *bufs,
                pltpu.SemaphoreType.DMA((len(parts), 2)),
            ],
        ),
        out_shape=jax.ShapeDtypeStruct((slot_rows, LANES, LANES), jnp.bfloat16),
        cost_estimate=pl.CostEstimate(
            flops=flops, bytes_accessed=2 * first * LANES * LANES, transcendentals=0
        ),
        name=f"grad_{first}",
    )(slots, *operands)


def bits_of(owners):
    return owners.bit_length() - 1


def chunks_of(total, most):
    number = -(-total // most)
    base, extra = divmod(total, number)
    out, at = [], 0
    for k in range(number):
        size = base + (1 if k < extra else 0)
        out.append((at, size))
        at += size
    return out


def scatter_body(owners, caps, jobs, *refs):
    stages = bits_of(owners)
    groups = len(caps)
    g_refs, small_ref = refs[:groups], refs[groups]
    out_refs, small_out = refs[groups + 1 : 2 * groups + 1], refs[2 * groups + 1]
    refs = refs[2 * groups + 2 :]
    landing = [refs[s * groups : (s + 1) * groups] for s in range(stages)]
    own, small_sum, small_land, send_sem, recv_sem, own_sem, small_send, small_recv = refs[
        stages * groups :
    ]
    me = lax.axis_index("dp")
    ten = lax.axis_index("tensor")
    bit = [(me // (1 << s)) % 2 for s in range(stages)]
    partner = [me + (1 - 2 * bit[s]) * (1 << s) for s in range(stages)]
    barrier = pltpu.get_barrier_semaphore()
    for s in range(stages):
        pl.semaphore_signal(barrier, inc=1, device_id=(partner[s], ten), device_id_type=MESH)
    pl.semaphore_signal(barrier, inc=1, device_id=(me, 1 - ten), device_id_type=MESH)
    pl.semaphore_wait(barrier, stages + 1)
    count = len(jobs)

    def small(s):
        to = (me, 1 - ten) if s == stages else (partner[s], ten)
        return pltpu.make_async_remote_copy(
            src_ref=small_ref if s == 0 else small_sum.at[s - 1],
            dst_ref=small_land.at[s],
            send_sem=small_send.at[s],
            recv_sem=small_recv.at[s],
            device_id=to,
            device_id_type=MESH,
        )

    def small_step(s):
        small(s).wait_recv()
        total = (small_ref[...] if s == 0 else small_sum[s - 1]) + small_land[s]
        if s == stages:
            small_out[...] = total
        else:
            small_sum[s] = total
            small(s + 1).start()

    small(0).start()

    def bit_at(s, k):
        if jobs[k][3] and s in (1, 2):
            return 3 - s
        return s

    def sides(s, k):
        before = owners >> s
        inner = 2 if jobs[k][3] and s == 1 else 1
        return before // 2 // inner, inner

    def part(s, k, which):
        g, at, size, _ = jobs[k]
        outer, inner = sides(s, k)
        span = pl.ds(at, size)
        if s == 0:
            return g_refs[g].at[:, which, span]
        ref = landing[s - 1][g]
        view = ref.reshape(outer, 2, inner, *ref.shape[1:])
        return view.at[:, which, :, span]

    def remote(s, k):
        g, at, size, _ = jobs[k]
        outer, inner = sides(s, k)
        span = pl.ds(at, size)
        b = bit_at(s, k)
        ref = landing[s][g]
        dst = ref.at[:, span] if s == 0 else ref.reshape(outer, inner, *ref.shape[1:]).at[:, :, span]
        return pltpu.make_async_remote_copy(
            src_ref=part(s, k, 1 - bit[b]),
            dst_ref=dst,
            send_sem=send_sem.at[s, k],
            recv_sem=recv_sem.at[s, k],
            device_id=(partner[b], ten),
            device_id_type=MESH,
        )

    def local(k):
        return pltpu.make_async_copy(
            part(0, k, bit[0]), own.at[k % 2, :, pl.ds(0, jobs[k][2])], own_sem.at[k % 2]
        )

    for k in range(count):
        remote(0, k).start()
    local(0).start()

    def work(s, k):
        g, at, size, _ = jobs[k]
        left = owners >> (s + 1)
        outer, inner = sides(s, k)
        if s == 0:
            if k + 1 < count:
                local(k + 1).start()
            local(k).wait()
        remote(s, k).wait_recv()
        mine_bit = bit[bit_at(s, k)]
        into = landing[s][g]

        def add(j, carry):
            o, u = j // size, j % size
            if s == 0:
                mine = own[k % 2, o, u]
            else:
                mine = landing[s - 1][g][(o // inner) * 2 * inner + mine_bit * inner + o % inner, at + u]
            total = into[o, at + u].astype(jnp.float32) + mine.astype(jnp.float32)
            if s == stages - 1:
                out_refs[g][at + u] = total
            else:
                into[o, at + u] = total.astype(jnp.bfloat16)
            return carry

        lax.fori_loop(0, left * size, add, 0)
        if s + 1 < stages:
            remote(s + 1, k).start()

    lag = 2
    for t in range(count + lag * (stages - 1)):
        for s in range(stages):
            k = t - lag * s
            if 0 <= k < count:
                work(s, k)
        if t % 2 == 1 and t // 2 <= stages:
            small_step(t // 2)
    for s in range(stages):
        for k in range(count):
            remote(s, k).wait_send()
    for s in range(stages + 1):
        small(s).wait_send()


def scatter_sum(units, small, owners, caps, collective=1, most=4):
    stages = bits_of(owners)
    depth, lanes = units[0].shape[1:]
    jobs = []
    for g, cap in enumerate(caps):
        for at, size in chunks_of(cap, most):
            jobs.append((g, at, size, stages > 2 and len(jobs) % 4 == 2))
    widest = max(size for _, _, size, _ in jobs)
    assert len(jobs) + 2 * (stages - 1) > 2 * stages + 1
    scratch = []
    for s in range(stages):
        for cap in caps:
            scratch.append(pltpu.VMEM((owners >> (s + 1), cap, depth, lanes), jnp.bfloat16))
    scratch += [
        pltpu.VMEM((2, owners // 2, widest, depth, lanes), jnp.bfloat16),
        pltpu.VMEM((stages, *small.shape), jnp.float32),
        pltpu.VMEM((stages + 1, *small.shape), jnp.float32),
        pltpu.SemaphoreType.DMA((stages, len(jobs))),
        pltpu.SemaphoreType.DMA((stages, len(jobs))),
        pltpu.SemaphoreType.DMA((2,)),
        pltpu.SemaphoreType.DMA((stages + 1,)),
        pltpu.SemaphoreType.DMA((stages + 1,)),
    ]
    return pl.pallas_call(
        functools.partial(scatter_body, owners, caps, tuple(jobs)),
        out_shape=[
            *[jax.ShapeDtypeStruct((cap, depth, lanes), jnp.float32) for cap in caps],
            jax.ShapeDtypeStruct(small.shape, jnp.float32),
        ],
        in_specs=[
            *[pl.BlockSpec(memory_space=pl.ANY)] * len(caps),
            pl.BlockSpec(memory_space=pltpu.VMEM),
        ],
        out_specs=[pl.BlockSpec(memory_space=pltpu.VMEM)] * (len(caps) + 1),
        scratch_shapes=scratch,
        compiler_params=pltpu.CompilerParams(collective_id=collective, has_side_effects=True),
        name="scatter_sum",
    )(
        *[group.reshape(owners // 2, 2, cap, depth, lanes) for group, cap in zip(units, caps)],
        small,
    )


def adam_values(master, one, two, gradient, rate):
    moment_one = BETA_ONE * one + (1.0 - BETA_ONE) * gradient
    moment_two = BETA_TWO * two + (1.0 - BETA_TWO) * gradient * gradient
    step_size = (
        moment_one
        / (1.0 - BETA_ONE**STEP)
        / (jnp.sqrt(moment_two / (1.0 - BETA_TWO**STEP)) + ADAM_EPS)
    )
    return master - rate * (step_size + WEIGHT_DECAY * master), moment_one, moment_two


def adam_step(opt_state, gradient, rate):
    return jnp.stack(adam_values(opt_state[0], opt_state[1], opt_state[2], gradient, rate))


def adam_body(scale, used_ref, state_ref, summed_ref, out_ref, *scratch):
    cap, rows, lanes = summed_ref.shape
    if scratch:
        scratch[0][...] = summed_ref[...].astype(jnp.float32)
        summed_ref = scratch[0]
    flat = summed_ref.reshape(cap * rows, lanes)
    used = used_ref[...] > 0
    for r in range(rows):
        here = slice(r * lanes, (r + 1) * lanes)
        summed = flat[pl.ds(r, cap, stride=rows), :] * scale
        gradient = jnp.where(used, summed, 0.0)
        new = adam_values(
            state_ref[0, :, here], state_ref[1, :, here], state_ref[2, :, here], gradient, LEARN_RATE
        )
        for k in range(3):
            out_ref[k, :, here] = new[k]


def adam_units(state, summed, slots, scale):
    cap, unit_width = state.shape[1:]
    mine = lax.axis_index("dp") * cap + jnp.arange(cap, dtype=jnp.int32)
    used = jnp.any(mine[:, None] == slots[None, :], axis=1).astype(jnp.int32)
    rows = 16
    block = rows * LANES
    return pl.pallas_call(
        functools.partial(adam_body, scale),
        grid=(unit_width // block,),
        in_specs=[
            pl.BlockSpec((cap, LANES), lambda i: (0, 0)),
            pl.BlockSpec((3, cap, block), lambda i: (0, 0, i)),
            pl.BlockSpec((cap, rows, LANES), lambda i: (0, i, 0)),
        ],
        out_specs=pl.BlockSpec((3, cap, block), lambda i: (0, 0, i)),
        out_shape=jax.ShapeDtypeStruct(state.shape, jnp.float32),
        scratch_shapes=[pltpu.VMEM((cap, rows, LANES), jnp.float32)]
        if summed.dtype == jnp.bfloat16
        else [],
        name=f"adam_{cap}",
    )(jnp.broadcast_to(used[:, None], (cap, LANES)), state, summed)


def spread_body(owners, cap, jobs, own_ref, out_ref, local_sem, send_sem, recv_sem):
    stages = bits_of(owners)
    me = lax.axis_index("dp")
    ten = lax.axis_index("tensor")
    bit = [(me // (1 << s)) % 2 for s in range(stages)]
    partner = [me + (1 - 2 * bit[s]) * (1 << s) for s in range(stages)]
    barrier = pltpu.get_barrier_semaphore()
    for s in range(stages):
        pl.semaphore_signal(barrier, inc=1, device_id=(partner[s], ten), device_id_type=MESH)
    pl.semaphore_wait(barrier, stages)
    tail = out_ref.shape[2:]

    def bit_at(s, k):
        b = stages - 1 - s
        return 3 - b if jobs[k][2] and b in (1, 2) else b

    def held(s, k):
        at, size, swapped = jobs[k]
        span = pl.ds(at, size)
        b = stages - 1 - s
        if swapped and b == 2:
            return out_ref.reshape(owners >> 3, 8, cap, *tail).at[:, me % 8, span]
        if swapped and b == 1:
            view = out_ref.reshape(owners >> 3, 2, 2, 2, cap, *tail)
            return view.at[:, bit[2], :, bit[0], span]
        low = 1 << (b + 1)
        return out_ref.reshape(owners // low, low, cap, *tail).at[:, me % low, span]

    def remote(s, k):
        b = bit_at(s, k)
        at, size, _ = jobs[k]
        dst = out_ref.at[me, pl.ds(at, size)] if s == 0 else held(s, k)
        return pltpu.make_async_remote_copy(
            src_ref=own_ref.at[pl.ds(at, size)] if s == 0 else dst,
            dst_ref=dst,
            send_sem=send_sem.at[s, k],
            recv_sem=recv_sem.at[s, k],
            device_id=(partner[b], ten),
            device_id_type=MESH,
        )

    local = pltpu.make_async_copy(own_ref, out_ref.at[me], local_sem.at[0])
    count = len(jobs)
    for k in range(count):
        remote(0, k).start()
    local.start()
    local.wait()
    for t in range(count + stages - 1):
        for s in range(stages):
            k = t - s
            if 0 <= k < count:
                remote(s, k).wait_recv()
                if s + 1 < stages:
                    remote(s + 1, k).start()
    for s in range(stages):
        for k in range(count):
            remote(s, k).wait_send()


def spread_units(own, owners, collective, most=4):
    cap, depth, lanes = own.shape
    stages = bits_of(owners)
    jobs = tuple(
        (at, size, stages > 2 and number % 4 == 2)
        for number, (at, size) in enumerate(chunks_of(cap, most))
    )
    out = pl.pallas_call(
        functools.partial(spread_body, owners, cap, jobs),
        out_shape=jax.ShapeDtypeStruct((owners, cap, depth, lanes), jnp.bfloat16),
        in_specs=[pl.BlockSpec(memory_space=pltpu.VMEM)],
        out_specs=pl.BlockSpec(memory_space=pl.ANY),
        scratch_shapes=[
            pltpu.SemaphoreType.DMA((1,)),
            pltpu.SemaphoreType.DMA((stages, len(jobs))),
            pltpu.SemaphoreType.DMA((stages, len(jobs))),
        ],
        compiler_params=pltpu.CompilerParams(collective_id=collective, has_side_effects=True),
        name=f"spread_{cap}",
    )(own)
    return out.reshape(owners * cap, depth, lanes)


def own_units(state, scale):
    cap, unit_width = state.shape[1:]
    return (state[0] * scale).reshape(cap, unit_width // LANES, LANES).astype(jnp.bfloat16)


def attend(query_f, key_f, query_s, key_s, lin_mask, win_mask):
    lin_score = jnp.einsum(
        "shf,thf->hst", query_f, key_f, preferred_element_type=jnp.float32
    ) / math.sqrt(FEAT)
    kernel = (1.0 + lin_score + 0.5 * lin_score * lin_score) * lin_mask
    lin_denom = jnp.sum(kernel, axis=-1, keepdims=True)
    lin_prob = kernel / lin_denom
    win_score = jnp.einsum(
        "shd,thd->hst", query_s, key_s, preferred_element_type=jnp.float32
    ) / math.sqrt(HEAD)
    inside = win_mask > 0
    win_peak = jnp.max(jnp.where(inside, win_score, NEG_FILL), axis=-1, keepdims=True)
    win_exp = jnp.exp(jnp.where(inside, win_score - win_peak, NEG_FILL))
    win_prob = win_exp / jnp.sum(win_exp, axis=-1, keepdims=True)
    return (lin_score, lin_denom, lin_prob, win_prob)


def per_device(
    inputs,
    cotangent,
    segments,
    slot_conv,
    slot_mix,
    slot_mlp,
    state_conv,
    state_mix,
    state_mlp,
    small_state,
):
    tensor_size = lax.axis_size("tensor")
    owners = lax.axis_size("dp")
    half_width = D // tensor_size
    local_heads = HEADS // tensor_size
    feat_cols = local_heads * FEAT
    ff_half = FF // tensor_size
    unit_width = state_conv.shape[2]
    cap_conv = state_conv.shape[1]
    cap_mix = state_mix.shape[1]
    cap_mlp = state_mlp.shape[1]
    own_conv, own_mix, own_mlp = lax.optimization_barrier(
        (
            own_units(state_conv, CONV_SCALE),
            own_units(state_mix, MIX_SCALE),
            own_units(state_mlp, MLP_SCALE),
        )
    )
    pooled = (
        spread_units(own_conv, owners, 2),
        lax.all_gather(own_mix, "dp", axis=0, tiled=True),
        lax.all_gather(own_mlp, "dp", axis=0, tiled=True),
    )
    per = D * LANES // unit_width
    narrow, middle = per * feat_cols // LANES, per * half_width // LANES
    wide = per * ff_half // LANES
    conv_pair, conv_back = lay_out(
        pooled[0], slot_conv, ((2 * middle, half_width, 7, 2), (middle, D, 7, 2))
    )
    conv_w = [conv_pair[:D], conv_pair[D:], conv_back]
    feat_pair, mix_trio, mix_back = lay_out(
        pooled[1],
        slot_mix,
        ((2 * narrow, feat_cols, 7, 2), (3 * middle, half_width, 7, 3), (middle, D, 7, 2)),
    )
    mix_w = [
        feat_pair[:D],
        feat_pair[D:],
        mix_trio[:D],
        mix_trio[D : 2 * D],
        mix_trio[2 * D :],
        mix_back,
    ]
    params = small_state[0] * SMALL_SCALE
    seg_ids = segments[0]
    length = seg_ids.shape[0]
    positions = jnp.arange(length)
    causal = (positions[:, None] >= positions[None, :]) & (seg_ids[:, None] == seg_ids[None, :])
    lin_mask = causal.astype(jnp.float32)
    win_mask = (causal & (positions[:, None] - positions[None, :] < WINDOW)).astype(jnp.float32)
    same_prev = [None]
    for shift_by in range(1, TAPS):
        earlier = jnp.pad(seg_ids, (shift_by, 0), constant_values=-1)[:length]
        same_prev.append((earlier == seg_ids).astype(jnp.float32)[:, None])
    column = lax.axis_index("tensor") * half_width
    taps_local = lax.dynamic_slice_in_dim(params[3:], column, half_width, 1)
    x_rows = inputs.astype(jnp.float32)
    normed_one = norm_rows(x_rows, params[0]).astype(jnp.bfloat16)
    conv_in = gather_rows(normed_one)
    value_c = product(conv_in, conv_w[0])
    gate_c = product(conv_in, conv_w[1])
    mixed_c = taps_local[0] * value_c
    for shift_by in range(1, TAPS):
        mixed_c = mixed_c + taps_local[shift_by] * delayed(value_c, shift_by) * same_prev[shift_by]
    gated_conv = (mixed_c * gate_c).astype(jnp.bfloat16)
    hidden_one = x_rows + sum_rows(product(gated_conv, conv_w[2]))
    normed_two = norm_rows(hidden_one, params[1]).astype(jnp.bfloat16)
    mix_in = gather_rows(normed_two)
    projected = [product(mix_in, weight).astype(jnp.bfloat16) for weight in mix_w[:5]]
    query_f = projected[0].reshape(length, local_heads, FEAT)
    key_f = projected[1].reshape(length, local_heads, FEAT)
    query_s = projected[2].reshape(length, local_heads, HEAD)
    key_s = projected[3].reshape(length, local_heads, HEAD)
    values_v = projected[4].reshape(length, local_heads, HEAD)
    _, _, lin_prob, win_prob = attend(query_f, key_f, query_s, key_s, lin_mask, win_mask)
    attended = jnp.einsum(
        "hst,thd->shd", lin_prob.astype(jnp.bfloat16), values_v, preferred_element_type=jnp.float32
    ) + jnp.einsum(
        "hst,thd->shd", win_prob.astype(jnp.bfloat16), values_v, preferred_element_type=jnp.float32
    )
    mix_out = attended.reshape(length, half_width).astype(jnp.bfloat16)
    hidden_two = hidden_one + sum_rows(product(mix_out, mix_w[5]))
    normed_three = norm_rows(hidden_two, params[2]).astype(jnp.bfloat16)
    ff_in = gather_rows(normed_three)
    back_three = gather_rows(cotangent)
    part_out, activated, back_gate, back_up, part_back = feed_forward(
        pooled[2], slot_mlp, wide, ff_in, back_three, ff_half
    )
    back_normed_three = sum_rows(part_back)
    mlp_units = grad_units(
        owners * cap_mlp,
        slot_mlp,
        (
            (ff_in, back_gate, 2 * LANES),
            (ff_in, back_up, 2 * LANES),
            (activated, back_three, LANES),
        ),
    )
    summed_mlp = lax.psum_scatter(mlp_units, "dp", scatter_dimension=0, tiled=True)
    result = (hidden_two + sum_rows(part_out)).astype(jnp.bfloat16)
    back_norm_three, gain_three = norm_back(hidden_two, params[2], back_normed_three)
    back_hidden_two = cotangent.astype(jnp.float32) + back_norm_three
    back_two = gather_rows(back_hidden_two.astype(jnp.bfloat16))
    back_attended = (
        product_right(back_two, mix_w[5]).astype(jnp.bfloat16).reshape(length, local_heads, HEAD)
    )
    lin_again, denom_again, lin_back, win_back = attend(
        query_f, key_f, query_s, key_s, lin_mask, win_mask
    )
    back_prob = jnp.einsum(
        "shd,thd->hst", back_attended, values_v, preferred_element_type=jnp.float32
    )
    back_values = jnp.einsum(
        "hst,shd->thd",
        lin_back.astype(jnp.bfloat16),
        back_attended,
        preferred_element_type=jnp.float32,
    ) + jnp.einsum(
        "hst,shd->thd",
        win_back.astype(jnp.bfloat16),
        back_attended,
        preferred_element_type=jnp.float32,
    )
    back_kernel = (back_prob - jnp.sum(back_prob * lin_back, axis=-1, keepdims=True)) / denom_again
    back_score = (back_kernel * (1.0 + lin_again) * lin_mask).astype(jnp.bfloat16)
    back_query_f = jnp.einsum(
        "hst,thf->shf", back_score, key_f, preferred_element_type=jnp.float32
    ) / math.sqrt(FEAT)
    back_key_f = jnp.einsum(
        "hst,shf->thf", back_score, query_f, preferred_element_type=jnp.float32
    ) / math.sqrt(FEAT)
    back_local = (
        win_back * (back_prob - jnp.sum(back_prob * win_back, axis=-1, keepdims=True))
    ).astype(jnp.bfloat16)
    back_query_s = jnp.einsum(
        "hst,thd->shd", back_local, key_s, preferred_element_type=jnp.float32
    ) / math.sqrt(HEAD)
    back_key_s = jnp.einsum(
        "hst,shd->thd", back_local, query_s, preferred_element_type=jnp.float32
    ) / math.sqrt(HEAD)
    back_projected = [
        piece_grad.reshape(length, -1).astype(jnp.bfloat16)
        for piece_grad in (back_query_f, back_key_f, back_query_s, back_key_s, back_values)
    ]
    back_normed_two = product_right(back_projected[0], mix_w[0])
    for piece_grad, weight in zip(back_projected[1:], mix_w[1:5]):
        back_normed_two = back_normed_two + product_right(piece_grad, weight)
    back_normed_two = sum_rows(back_normed_two)
    back_norm_two, gain_two = norm_back(hidden_one, params[1], back_normed_two)
    back_hidden_one = back_hidden_two + back_norm_two
    mix_units = grad_units(
        owners * cap_mix,
        slot_mix,
        (
            (mix_in, back_projected[0], 7 * LANES),
            (mix_in, back_projected[1], 7 * LANES),
            *[(mix_in, piece_grad, 2 * LANES) for piece_grad in back_projected[2:]],
            (mix_out, back_two, LANES),
        ),
    )
    back_one = gather_rows(back_hidden_one.astype(jnp.bfloat16))
    back_gated = product_right(back_one, conv_w[2])
    back_mixed = back_gated * gate_c
    back_gate_c = (back_gated * mixed_c).astype(jnp.bfloat16)
    back_value_f = taps_local[0] * back_mixed
    tap_grads = [jnp.sum(back_mixed * value_c, axis=0)]
    for shift_by in range(1, TAPS):
        masked = back_mixed * same_prev[shift_by]
        back_value_f = back_value_f + taps_local[shift_by] * advanced(masked, shift_by)
        tap_grads.append(jnp.sum(masked * delayed(value_c, shift_by), axis=0))
    back_value_c = back_value_f.astype(jnp.bfloat16)
    back_normed_one = sum_rows(
        product_right(back_value_c, conv_w[0]) + product_right(back_gate_c, conv_w[1])
    )
    back_norm_one, gain_one = norm_back(x_rows, params[0], back_normed_one)
    grad_input = back_hidden_one + back_norm_one
    conv_units = grad_units(
        owners * cap_conv,
        slot_conv,
        (
            (conv_in, back_value_c, 2 * LANES),
            (conv_in, back_gate_c, 2 * LANES),
            (gated_conv, back_one, LANES),
        ),
    )
    taps_full = lax.dynamic_update_slice(
        jnp.zeros((TAPS, D), jnp.float32), jnp.stack(tap_grads), (jnp.int32(0), column)
    )
    small_grad = jnp.concatenate([jnp.stack([gain_one, gain_two, gain_three]), taps_full], axis=0)
    summed_mix, summed_conv, small_summed = scatter_sum(
        (mix_units, conv_units), small_grad, owners, (cap_mix, cap_conv)
    )
    new_conv = adam_units(state_conv, summed_conv, slot_conv, CONV_SCALE / owners)
    new_mix = adam_units(state_mix, summed_mix, slot_mix, MIX_SCALE / owners)
    new_mlp = adam_units(state_mlp, summed_mlp, slot_mlp, MLP_SCALE / owners)
    small_new = adam_step(small_state, small_summed * (SMALL_SCALE / owners), SMALL_RATE)
    return (
        result,
        grad_input,
        new_conv,
        new_mix,
        new_mlp,
        small_new[1:],
        small_new[0] - small_state[0],
    )


def solution(mesh):
    placed = (
        P(("dp", "tensor"), None),
        P(("dp", "tensor"), None),
        P("dp", None),
        P(),
        P(),
        P(),
        P(None, "dp", "tensor"),
        P(None, "dp", "tensor"),
        P(None, "dp", "tensor"),
        P(),
    )
    return jax.shard_map(
        per_device,
        mesh=mesh,
        in_specs=placed,
        out_specs=(
            P(("dp", "tensor"), None),
            P(("dp", "tensor"), None),
            P(None, "dp", "tensor"),
            P(None, "dp", "tensor"),
            P(None, "dp", "tensor"),
            P(),
            P(),
        ),
        check_vma=False,
    )
```
